512 devices in a mesh: depth: 32 (over x, y, core), area: 16 (over z).
Axes of the slice: x: 4, y: 4, z: 16, core: 2. Of those that a mesh axis runs over, the one named last changes fastest.
Arguments:
- rhs_field: float32 [64, 32, 8192], P('depth', None, 'area'), may hold values from -8 to 8
- start_field: float32 [64, 32, 8192], P('depth', None, 'area'), may hold values from -4 to 4
- inverses: float32 [64, 8192, 512], P('depth', 'area'), may hold values from -0.044194174 to 1
- facies: int32 [64, 8192], P('depth', 'area'), may hold values from 0 to 7
- neighbours: int32 [8192, 4], P('area'), may hold values from 0 to 639, as said below
- lateral_table: float32 [8, 4], replicated, may hold values from 0.05 to 0.3
- vertical_table: float32 [8], replicated, may hold values from 0.9 to 1
Outputs:
- updated: float32 [64, 32, 8192], P('depth', None, 'area')
The draws below stay inside these ranges and needn't reach their ends.
Inputs may be any that keep to these rules, and one draw needn't show every extreme that they name: `neighbours`: index 64 + c is column c itself; entries 0 and 1 of column c are c - 1 and c + 1, the others lie within 64 columns of c and differ from it.
All inputs are finite; a program needn't handle non-finite values.
Results may differ from the reference program's by a relative error of at most 0.00016.
Values sent between devices are 32-bit elements; how exact they have to be, the bound alone decides.
A program may use at most 128 MiB of HBM per device.

```python
import math
import jax
import jax.numpy as jnp
from jax import lax

CELLS = 512
RHS = 32
HW = 64
NBRS = 4
FACIES = 8
LAYERS = 64
NCELLS = 8192


def draw_neighbours(key, part):
    cell = jnp.arange(NCELLS, dtype=jnp.int32) % CELLS
    first, second = jax.random.split(jax.random.fold_in(key, 11))
    reach = jax.random.randint(first, (NCELLS, NBRS - 2), 1, HW + 1)
    sign = jax.random.randint(second, (NCELLS, NBRS - 2), 0, 2) * 2 - 1
    left = jnp.full((NCELLS, 1), -1, jnp.int32)
    right = jnp.full((NCELLS, 1), 1, jnp.int32)
    offsets = jnp.concatenate([left, right, reach * sign], axis=1)
    return (HW + cell[:, None] + offsets).astype(jnp.int32)


def draw_inverses(key, part):
    first, second = jax.random.split(jax.random.fold_in(key, 23))
    blocks = NCELLS // CELLS
    diag = jnp.exp(jax.random.uniform(first, (LAYERS, blocks, CELLS), jnp.float32, math.log(0.9), 0.0))
    eye = jnp.eye(CELLS, dtype=jnp.float32)
    off = jnp.clip(jax.random.normal(second, (LAYERS, blocks, CELLS, CELLS), jnp.float32), -4.0, 4.0) * (0.25 / math.sqrt(CELLS))
    whole = off * (1.0 - eye)[None, None] + eye[None, None] * diag[..., None]
    return whole.reshape(LAYERS, NCELLS, CELLS)


def place_ends(values, key, least, high):
    longest = values.shape.index(max(values.shape))
    spots = []
    for shift in (0, 1):
        where = [jax.random.randint(jax.random.fold_in(key, axis), (), 0, length) for axis, length in enumerate(values.shape)]
        where[longest] = (where[longest] + shift) % values.shape[longest]
        spots.append(tuple(where))
    return values.at[spots[0]].set(least).at[spots[1]].set(high)


def steps_of(key, shape, shards, smallest, high):
    loudness = 1.0
    for dim, shards_of in shards:
        heights = jax.random.uniform(jax.random.fold_in(jax.random.fold_in(key, 6), dim), (shards_of,), jnp.float32, smallest / len(shards), high / len(shards))
        loudness = loudness * jnp.repeat(jnp.exp(heights), shape[dim] // shards_of).reshape((-1,) + (1,) * (len(shape) - 1 - dim))
    return loudness


def noise(own_key, extent, width, most, pieces=(), kind=jnp.bfloat16):
    array = width * jax.random.normal(own_key, extent, jnp.float32)
    if pieces:
        array = array * steps_of(own_key, extent, pieces, -0.22, 0.18)
    return jnp.clip(array, -most, most).astype(kind)


def setup_inputs(seed: int = 0) -> dict:
    streams_of = jax.random.split(jax.random.key(seed), 8)
    return {
        "rhs_field": noise(streams_of[0], (LAYERS, RHS, NCELLS), 1.0, 8.0, ((0, 32), (2, 16)), jnp.float32),
        "start_field": noise(streams_of[1], (LAYERS, RHS, NCELLS), 0.5, 4.0, ((0, 32), (2, 16)), jnp.float32),
        "inverses": draw_inverses(jax.random.fold_in(streams_of[7], 71), 0),
        "facies": place_ends(jax.random.randint(streams_of[3], (LAYERS, NCELLS), 0, FACIES), jax.random.fold_in(streams_of[3], 1), 0, FACIES - 1).astype(jnp.int32),
        "neighbours": draw_neighbours(jax.random.fold_in(streams_of[7], 71), 0),
        "lateral_table": jnp.clip(jnp.exp(jax.random.uniform(streams_of[5], (FACIES, NBRS), jnp.float32, math.log(0.05), math.log(0.3))), 0.05, 0.3),
        "vertical_table": jnp.clip(jnp.exp(jax.random.uniform(streams_of[6], (FACIES,), jnp.float32, math.log(0.9), math.log(1.0))), 0.9, 1.0),
    }


def apply_blocks(field, blocks):
    parts = field.reshape(field.shape[0], -1, CELLS)
    mats = blocks.reshape(-1, CELLS, CELLS)
    return jnp.einsum("rac,acd->rad", parts, mats, precision=lax.Precision.HIGHEST).reshape(field.shape)


def apply_blocks_t(field, blocks):
    parts = field.reshape(field.shape[0], -1, CELLS)
    mats = blocks.reshape(-1, CELLS, CELLS)
    return jnp.einsum("rad,acd->rac", parts, mats, precision=lax.Precision.HIGHEST).reshape(field.shape)


def lateral(field, facies, neighbours, lateral_table):
    starts = (jnp.arange(NCELLS, dtype=jnp.int32) // CELLS * CELLS)[:, None]
    index = (starts + neighbours).astype(jnp.int32)

    def one_layer(pair):
        layer, kinds = pair
        padded = jnp.pad(layer, ((0, 0), (HW, HW)))
        values = padded[:, index]
        weight = lateral_table[kinds]
        return jnp.sum(weight[None] * (layer[:, :, None] - values), axis=-1)

    return lax.map(one_layer, (field, facies))


def reference(rhs_field, start_field, inverses, facies, neighbours, lateral_table, vertical_table):
    vert = vertical_table[facies]
    zero_layer = jnp.zeros((1, RHS, NCELLS), jnp.float32)
    upper = jnp.concatenate([vert[1:, None, :] * start_field[1:], zero_layer], axis=0)
    g = rhs_field - lateral(start_field, facies, neighbours, lateral_table) + upper

    def down(carry, item):
        g_k, vert_k, inv_k = item
        y_k = apply_blocks(g_k + vert_k[None] * carry, inv_k)
        return y_k, y_k

    _, y = lax.scan(down, jnp.zeros((RHS, NCELLS), jnp.float32), (g, vert, inverses))
    y_prev = jnp.concatenate([zero_layer, y[:-1]], axis=0)
    h = rhs_field - lateral(y, facies, neighbours, lateral_table) + vert[:, None, :] * y_prev

    def upward(carry, item):
        h_k, vert_k, inv_k = item
        z_k = apply_blocks_t(h_k + carry, inv_k)
        return vert_k[None] * z_k, z_k

    _, updated = lax.scan(upward, jnp.zeros((RHS, NCELLS), jnp.float32), (h, vert, inverses), reverse=True)
    return updated
```

```python
import functools

import jax
import jax.numpy as jnp
from jax import lax
from jax.experimental import pallas as pl
from jax.experimental.pallas import tpu as pltpu
from jax.sharding import PartitionSpec as P

MESH = pl.DeviceIdType.MESH
F32 = jnp.float32
BF16 = jnp.bfloat16
HW = 64
LANES = 128
ROW = 8
HUB = ROW - 1
BLOCKS = 8

SENDS = (
    "start_right", "start_left", "below", "f_next", "down_hub", "down6",
    "down5", "down3", "down1", "down_pair", "y_right", "y_left",
    "w_pair", "w_hub", "g_prev", "up_hub", "up6", "up5",
    "up3", "up1", "up_pair",
)
RECVS = (
    "start_lo", "start_hi", "below", "f", "down", "y_lo",
    "y_hi", "w_pair", "w0", "w1", "w2", "g",
    "up",
)


def split(x):
    high = x.astype(BF16)
    return high, (x - high.astype(F32)).astype(BF16)


def dot3(x, w_high, w_low, transposed=False):
    high, low = split(x)
    dims = (((1,), (1 if transposed else 0,)), ((), ()))
    rows = x.shape[0]
    both = lax.dot_general(
        jnp.concatenate([high, low], axis=0), w_high, dims, preferred_element_type=F32
    )
    rest = lax.dot_general(high, w_low, dims, preferred_element_type=F32)
    return both[:rows] + both[rows:] + rest


def kernel(
    depth, areas,
    lat_tab, vert_tab, facies, nbrs, rhs_hbm, start_hbm, inv_hbm,
    out,
    rhs, start, inv, dh, dl, th, tl, ina, ah, al, outa, ins, sh, sl, outs, mh, ml,
    lat_h, lat_l, wts, wsum, vert, slo, shi, ylo, yhi, below_out, below_in,
    g, f_in, f_out, o_buf, eb, e_next, e_in, y, h, p_buf, w_out, w_pair, w_hub, o_up,
    g_in, g_out, ub, u_next,
    local, snd, rcv, snd_a, rcv_a, snd_s, rcv_s,
):
    rows = depth // ROW
    d = lax.axis_index("depth")
    z = lax.axis_index("area")
    r, c = d // ROW, d % ROW
    width = out.shape[2]
    count = out.shape[1]
    tiles = width // LANES
    size = width // BLOCKS
    base = r * ROW
    waits = []

    def both(*conds):
        return functools.reduce(jnp.logical_and, conds)

    def copy(src, dst, send, recv, depth_id, area_id=None):
        return pltpu.make_async_remote_copy(
            src_ref=src,
            dst_ref=dst,
            send_sem=snd.at[SENDS.index(send)],
            recv_sem=rcv.at[RECVS.index(recv)],
            device_id=(depth_id, z if area_id is None else area_id),
            device_id_type=MESH,
        )

    def send(cond, args):
        waits.append((cond, args))
        copy(*args()).start()

    def received(dst, recv):
        copy(dst, dst, SENDS[0], recv, d).wait_recv()

    def block_a(b):
        return pltpu.make_async_remote_copy(
            src_ref=outa.at[b], dst_ref=ina.at[b], send_sem=snd_a.at[b], recv_sem=rcv_a.at[b],
            device_id=(d + 1, z), device_id_type=MESH,
        )

    def block_s(b):
        return pltpu.make_async_remote_copy(
            src_ref=outs.at[b], dst_ref=ins.at[b], send_sem=snd_s.at[b], recv_sem=rcv_s.at[b],
            device_id=(d - 1, z), device_id_type=MESH,
        )

    loads = [
        pltpu.make_async_copy(start_hbm, start, local.at[0]),
        pltpu.make_async_copy(inv_hbm.at[1], inv.at[1], local.at[1]),
        pltpu.make_async_copy(inv_hbm.at[0], inv.at[0], local.at[2]),
        pltpu.make_async_copy(rhs_hbm, rhs, local.at[3]),
    ]
    for load in loads:
        load.start()

    barrier = pltpu.get_barrier_semaphore()
    is_spoke = both(c % 2 == 1, c < HUB)
    partners = [
        (d > 0, d - 1, z),
        (d < depth - 1, d + 1, z),
        (z > 0, d, z - 1),
        (z < areas - 1, d, z + 1),
        (is_spoke, base + HUB, z),
        (both(c == HUB, r > 0), d - ROW, z),
        (both(c == HUB, r < rows - 1), d + ROW, z),
    ] + [(c == HUB, base + spoke, z) for spoke in (1, 3, 5)]
    for cond, to_depth, to_area in partners:

        @pl.when(cond)
        def _():
            pl.semaphore_signal(
                barrier, inc=1, device_id=(to_depth, to_area), device_id_type=MESH
            )

    kinds = facies[...]
    facies_count = lat_tab.shape[1]
    v_rows = jnp.zeros(kinds.shape, F32)
    w_rows = [jnp.zeros(kinds.shape, F32) for _ in range(lat_tab.shape[0])]
    for kind in range(facies_count):
        mask = kinds == kind
        v_rows = jnp.where(mask, vert_tab[kind], v_rows)
        w_rows = [jnp.where(mask, lat_tab[j, kind], w) for j, w in enumerate(w_rows)]
    vert[...] = v_rows
    for j, w in enumerate(w_rows):
        wts[j] = w
    wsum[...] = functools.reduce(jnp.add, w_rows)

    for t in range(tiles):
        lanes = slice(t * LANES, (t + 1) * LANES)
        for k in range(2):
            for first in (0, 2 * LANES + HW):
                lat_h[k, t, first : first + HW, :] = jnp.zeros((HW, LANES), BF16)
                lat_l[k, t, first : first + HW, :] = jnp.zeros((HW, LANES), BF16)
        for first in range(HW, 2 * LANES + HW, HW):
            place = lax.broadcasted_iota(jnp.int32, (HW, LANES), 0) + (first + t * LANES - HW)
            sums = [jnp.zeros((HW, LANES), F32) for _ in range(2)]
            for j in range(nbrs.shape[0]):
                hit = place == nbrs[j : j + 1, lanes]
                for k in range(2):
                    sums[k] = sums[k] + jnp.where(hit, wts[j, k : k + 1, lanes], 0.0)
            for k in range(2):
                high, low = split(sums[k])
                lat_h[k, t, first : first + HW, :] = high
                lat_l[k, t, first : first + HW, :] = low

    def lateral(k, v, low, high):
        parts = [low[k]] + [v[:, t * LANES : (t + 1) * LANES] for t in range(tiles)] + [high[k]]
        sums = [
            dot3(jnp.concatenate(parts[t : t + 3], axis=1), lat_h[k, t], lat_l[k, t])
            for t in range(tiles)
        ]
        return wsum[k : k + 1, :] * v - jnp.concatenate(sums, axis=1)

    loads[0].wait()
    below_out[...] = vert[0:1, :] * start[0]
    partner_count = sum(cond.astype(jnp.int32) for cond, _, _ in partners)
    pl.semaphore_wait(barrier, partner_count)

    has_left, has_right = z > 0, z < areas - 1

    def halo(field, low, high, name):
        @pl.when(has_right)
        def _():
            send(lambda: has_right, lambda: (
                field.at[:, :, pl.ds(width - LANES, LANES)], low,
                name + "_right", name + "_lo", d, z + 1,
            ))

        @pl.when(has_left)
        def _():
            send(lambda: has_left, lambda: (
                field.at[:, :, pl.ds(0, LANES)], high,
                name + "_left", name + "_hi", d, z - 1,
            ))

        @pl.when(jnp.logical_not(has_left))
        def _():
            low[...] = jnp.zeros(low.shape, F32)

        @pl.when(jnp.logical_not(has_right))
        def _():
            high[...] = jnp.zeros(high.shape, F32)

    def halo_received(low, high, name):
        @pl.when(has_left)
        def _():
            received(low, name + "_lo")

        @pl.when(has_right)
        def _():
            received(high, name + "_hi")

    halo(start, slo, shi, "start")

    @pl.when(d > 0)
    def _():
        send(lambda: d > 0, lambda: (below_out, below_in, "below", "below", d - 1))

    def split_layer(k):
        def body(i, _):
            some = pl.ds(pl.multiple_of(i * LANES, LANES), LANES)
            high, low = split(inv[k, some, :])
            dh[k, some, :] = high
            dl[k, some, :] = low
            return 0

        lax.fori_loop(0, tiles, body, 0)

    per_tile = LANES // size
    loads[1].wait()
    split_layer(1)
    loads[2].wait()

    def compose(i, _):
        some = pl.ds(pl.multiple_of(i * LANES, LANES), LANES)
        scale = jnp.transpose(jnp.broadcast_to(vert[0:1, some], (LANES, LANES)))
        left = inv[0, some, :] * vert[1:2, :] * jnp.concatenate([scale] * tiles, axis=1)
        product = dot3(left, dh[1], dl[1])
        high, low = split(product)
        th[some, :] = high
        tl[some, :] = low
        for part in range(per_tile):
            outa[i * per_tile + part] = product[part * size : (part + 1) * size]

        @pl.when(c == 0)
        def _():
            for part in range(per_tile):
                block_a(i * per_tile + part).start()

        return 0

    lax.fori_loop(0, tiles, compose, 0)

    @pl.when(c == HUB)
    def _():
        def body(i, _):
            some = pl.ds(pl.multiple_of(i * LANES, LANES), LANES)
            turned = jnp.transpose(outa[:, :, some].reshape(width, LANES))
            for part in range(per_tile):
                outs[i * per_tile + part] = turned[part * size : (part + 1) * size]
                block_s(i * per_tile + part).start()
            return 0

        lax.fori_loop(0, tiles, body, 0)

    split_layer(0)

    loads[3].wait()
    halo_received(slo, shi, "start")

    @pl.when(d < depth - 1)
    def _():
        received(below_in, "below")

    @pl.when(d == depth - 1)
    def _():
        below_in[...] = jnp.zeros(below_in.shape, F32)

    g[0] = rhs[0] - lateral(0, start[0], slo, shi) + vert[1:2, :] * start[1]
    g[1] = rhs[1] - lateral(1, start[1], slo, shi) + below_in[...]
    first = dot3(g[0], dh[0], dl[0])
    o_buf[...] = dot3(g[1] + vert[1:2, :] * first, dh[1], dl[1])

    @pl.when(c == 0)
    def _():
        f_in[...] = jnp.zeros(f_in.shape, F32)
        f_out[...] = o_buf[...]

    step_a = (c // 2) * 4 + c % 2
    last = HUB - c
    step_s = (last // 2) * 4 + last % 2

    def next_f():
        return f_out, f_in, "f_next", "f", d + 1

    def first_down():
        return f_out, eb, "down_hub", "down", d + ROW

    def slot(s, _):
        @pl.when(both(c > 0, s >= step_a, s < step_a + BLOCKS))
        def _():
            b = s - step_a
            some = pl.ds(pl.multiple_of(b * size, size), size)
            block_a(b).wait_recv()
            x = ina[b]
            high, low = split(x)
            ah[some, :] = high
            al[some, :] = low
            product = dot3(x, th[...], tl[...])
            outa[b] = product

            @pl.when(c < HUB)
            def _():
                block_a(b).start()

            @pl.when(c == HUB)
            def _():
                high, low = split(product)
                mh[some, :] = high
                ml[some, :] = low

        @pl.when(s == step_a + 2)
        def _():
            @pl.when(c > 0)
            def _():
                received(f_in, "f")
                f_out[...] = dot3(f_in[...], th[...], tl[...]) + o_buf[...]

            @pl.when(c < HUB)
            def _():
                copy(*next_f()).start()

            @pl.when(both(c == HUB, r == 0))
            def _():
                copy(*first_down()).start()

        @pl.when(both(c < HUB, s >= step_s, s < step_s + BLOCKS))
        def _():
            b = s - step_s
            some = pl.ds(pl.multiple_of(b * size, size), size)
            block_s(b).wait_recv()
            x = ins[b]
            high, low = split(x)
            sh[some, :] = high
            sl[some, :] = low

            @pl.when(c > 0)
            def _():
                outs[b] = dot3(x, th[...], tl[...], True)
                block_s(b).start()

        return 0

    lax.fori_loop(0, (ROW // 2 - 1) * 4 + 1 + BLOCKS, slot, 0)
    waits.append((lambda: c < HUB, next_f))
    waits.append((lambda: both(c == HUB, r == 0), first_down))

    def spread(cond, buf, name):
        @pl.when(c == HUB)
        def _():
            for spoke in (3, 1, 5, 6):
                send(
                    lambda: both(cond(), c == HUB),
                    lambda spoke=spoke: (buf, buf, name + str(spoke), name, base + spoke),
                )

        @pl.when(is_spoke)
        def _():
            send(lambda: both(cond(), is_spoke), lambda: (buf, buf, name + "_pair", name, d - 1))

    @pl.when(r == 0)
    def _():
        e_in[...] = f_in[...]

    @pl.when(r > 0)
    def _():
        received(eb, "down")
        spread(lambda: r > 0, eb, "down")

        @pl.when(both(c == HUB, r < rows - 1))
        def _():
            e_next[...] = dot3(eb[...], mh[...], ml[...]) + f_out[...]
            send(
                lambda: both(c == HUB, r > 0, r < rows - 1),
                lambda: (e_next, eb, "down_hub", "down", d + ROW),
            )

        @pl.when(c == 0)
        def _():
            e_in[...] = eb[...]

        @pl.when(c > 0)
        def _():
            e_in[...] = dot3(eb[...], ah[...], al[...]) + f_in[...]

    entering = vert[0:1, :] * e_in[...]
    y[0] = dot3(g[0] + entering, dh[0], dl[0])
    y[1] = dot3(g[1] + vert[1:2, :] * y[0], dh[1], dl[1])
    halo(y, ylo, yhi, "y")
    halo_received(ylo, yhi, "y")
    h[0] = rhs[0] - lateral(0, y[0], ylo, yhi) + vert[0:1, :] * e_in[...]
    h[1] = rhs[1] - lateral(1, y[1], ylo, yhi) + vert[1:2, :] * y[0]

    above = dot3(h[1], dh[1], dl[1], True)
    p_buf[...] = vert[0:1, :] * dot3(h[0] + vert[1:2, :] * above, dh[0], dl[0], True)

    @pl.when(r > 0)
    def _():
        @pl.when(c == 0)
        def _():
            w_out[...] = p_buf[...]

        @pl.when(c > 0)
        def _():
            w_out[...] = dot3(p_buf[...], ah[...], al[...], True)

        @pl.when(c % 2 == 0)
        def _():
            send(
                lambda: both(r > 0, c % 2 == 0),
                lambda: (w_out, w_pair, "w_pair", "w_pair", d + 1),
            )

        @pl.when(c % 2 == 1)
        def _():
            received(w_pair, "w_pair")
            w_out[...] = w_out[...] + w_pair[...]

        for spoke in (1, 3, 5):

            @pl.when(c == spoke)
            def _():
                send(
                    lambda spoke=spoke: both(r > 0, c == spoke),
                    lambda i=spoke // 2: (w_out, w_hub.at[i], "w_hub", "w" + str(i), base + HUB),
                )

        @pl.when(c == HUB)
        def _():
            for spoke in range(3):
                received(w_hub.at[spoke], "w" + str(spoke))
            o_up[...] = w_out[...] + (w_hub[0] + (w_hub[1] + w_hub[2]))

            @pl.when(r == rows - 1)
            def _():
                send(
                    lambda: both(c == HUB, r > 0, r == rows - 1),
                    lambda: (o_up, ub, "up_hub", "up", d - ROW),
                )

    @pl.when(c == HUB)
    def _():
        g_in[...] = jnp.zeros(g_in.shape, F32)
        g_out[...] = p_buf[...]

    @pl.when(c < HUB)
    def _():
        received(g_in, "g")
        g_out[...] = dot3(g_in[...], th[...], tl[...], True) + p_buf[...]

    @pl.when(c > 0)
    def _():
        send(lambda: c > 0, lambda: (g_out, g_in, "g_prev", "g", d - 1))

    @pl.when(r < rows - 1)
    def _():
        received(ub, "up")
        spread(lambda: r < rows - 1, ub, "up")

        @pl.when(both(c == HUB, r > 0))
        def _():
            u_next[...] = dot3(ub[...], mh[...], ml[...], True) + o_up[...]
            send(
                lambda: both(c == HUB, r > 0, r < rows - 1),
                lambda: (u_next, ub, "up_hub", "up", d - ROW),
            )

        @pl.when(c == HUB)
        def _():
            g_in[...] = ub[...]

        @pl.when(c < HUB)
        def _():
            g_in[...] = g_in[...] + dot3(ub[...], sh[...], sl[...])

    upper = dot3(h[1] + g_in[...], dh[1], dl[1], True)
    out[1] = upper
    out[0] = dot3(h[0] + vert[1:2, :] * upper, dh[0], dl[0], True)

    for cond, args in waits:
        @pl.when(cond())
        def _():
            copy(*args()).wait_send()

    @pl.when(c < HUB)
    def _():
        for b in range(BLOCKS):
            block_a(b).wait_send()

    @pl.when(c > 0)
    def _():
        for b in range(BLOCKS):
            block_s(b).wait_send()


def shards(depth, areas, rhs_field, start_field, inverses, facies, neighbours, lateral_table, vertical_table):
    layers, count, width = rhs_field.shape
    size = width // BLOCKS
    tiles = width // LANES
    field = (layers, count, width)
    matrix = (width, width)
    state = pltpu.VMEM((count, width), F32)

    def blocks():
        return pltpu.VMEM((BLOCKS, size, width), F32)

    def halves():
        return [pltpu.VMEM(matrix, BF16)] * 2

    halo = pltpu.VMEM((layers, count, LANES), F32)
    scratch = (
        [pltpu.VMEM(field, F32)] * 2
        + [pltpu.VMEM((layers,) + matrix, F32)]
        + [pltpu.VMEM((layers,) + matrix, BF16)] * 2
        + halves()
        + [blocks()] + halves() + [blocks()]
        + [blocks()] + halves() + [blocks()]
        + halves()
        + [pltpu.VMEM((layers, tiles, 3 * LANES, LANES), BF16)] * 2
        + [pltpu.VMEM((neighbours.shape[1], layers, width), F32)]
        + [pltpu.VMEM((layers, width), F32)] * 2
        + [halo] * 4
        + [state] * 2
        + [pltpu.VMEM(field, F32)] + [state] * 3
        + [state] * 3
        + [pltpu.VMEM(field, F32)] * 2
        + [state] * 3
        + [pltpu.VMEM((3, count, width), F32)] + [state]
        + [state] * 4
        + [
            pltpu.SemaphoreType.DMA((4,)),
            pltpu.SemaphoreType.DMA((len(SENDS),)),
            pltpu.SemaphoreType.DMA((len(RECVS),)),
        ]
        + [pltpu.SemaphoreType.DMA((BLOCKS,))] * 4
    )
    vmem = pl.BlockSpec(memory_space=pltpu.VMEM)
    smem = pl.BlockSpec(memory_space=pltpu.SMEM)
    hbm = pl.BlockSpec(memory_space=pl.ANY)
    return pl.pallas_call(
        functools.partial(kernel, depth, areas),
        out_shape=jax.ShapeDtypeStruct(field, F32),
        in_specs=[smem, smem, vmem, vmem, hbm, hbm, hbm],
        out_specs=vmem,
        scratch_shapes=scratch,
        compiler_params=pltpu.CompilerParams(
            collective_id=0, has_side_effects=True, vmem_limit_bytes=60 * 1024 * 1024
        ),
        name="sweep",
    )(lateral_table.T, vertical_table, facies, neighbours.T, rhs_field, start_field, inverses)


def solution(mesh):
    return jax.shard_map(
        functools.partial(shards, mesh.shape["depth"], mesh.shape["area"]),
        mesh=mesh,
        in_specs=(
            P("depth", None, "area"),
            P("depth", None, "area"),
            P("depth", "area", None),
            P("depth", "area"),
            P("area", None),
            P(),
            P(),
        ),
        out_specs=P("depth", None, "area"),
        check_vma=False,
    )
```

```python
import functools

import jax
import jax.numpy as jnp
from jax import lax
from jax.experimental import pallas as pl
from jax.experimental.pallas import tpu as pltpu
from jax.sharding import PartitionSpec as P

MESH = pl.DeviceIdType.MESH
F32 = jnp.float32
BF16 = jnp.bfloat16
HW = 64
LANES = 128
ROW = 8
LAST = ROW - 1
HUB = 3
SPOKES = (7, 1, 5)
BLOCKS = 8

SENDS = (
    "start_right", "start_left", "below", "f_next", "o_hub", "down_hub",
    "down7", "down1", "down5", "down2", "down_pair", "y_right",
    "y_left", "w_pair", "w_hub", "g_prev", "up_hub", "up7",
    "up1", "up5", "up2", "up_pair",
)
RECVS = (
    "start_lo", "start_hi", "below", "f", "o", "down",
    "y_lo", "y_hi", "w_pair", "w0", "w1", "w2",
    "g", "up",
)


def split(x):
    high = x.astype(BF16)
    return high, (x - high.astype(F32)).astype(BF16)


def dot3(x, w_high, w_low, transposed=False):
    return dot_halves(*split(x), w_high, w_low, transposed)


def dot_halves(high, low, w_high, w_low, transposed):
    dims = (((1,), (1 if transposed else 0,)), ((), ()))
    rows = high.shape[0]
    both = lax.dot_general(
        jnp.concatenate([high, low], axis=0), w_high, dims, preferred_element_type=F32
    )
    rest = lax.dot_general(high, w_low, dims, preferred_element_type=F32)
    return both[:rows] + both[rows:] + rest


def kernel(
    depth, areas,
    lat_tab, vert_tab, facies, nbrs, rhs_hbm, start_hbm, inv_hbm,
    out,
    rhs, start, inv, dh, dl, th, tl, ina, ah, al, outa, ins, sh, sl, outs, bh, bl, mh, ml,
    lat_h, lat_l, wts, wsum, vert, slo, shi, ylo, yhi, to_right, to_left, below_out, below_in,
    g, f_in, f_out, o_buf, o_down, eb, e_next, e_in, y, h, p_buf, w_out, w_pair, w_hub, o_up,
    g_in, g_out, ub, u_next,
    local, snd, rcv, snd_a, rcv_a, snd_s, rcv_s,
):
    rows = depth // ROW
    d = lax.axis_index("depth")
    z = lax.axis_index("area")
    r, c = d // ROW, d % ROW
    width = out.shape[2]
    count = out.shape[1]
    tiles = width // LANES
    size = width // BLOCKS
    base = r * ROW
    waits = []

    def both(*conds):
        return functools.reduce(jnp.logical_and, conds)

    def copy(src, dst, send, recv, depth_id, area_id=None):
        return pltpu.make_async_remote_copy(
            src_ref=src,
            dst_ref=dst,
            send_sem=snd.at[SENDS.index(send)],
            recv_sem=rcv.at[RECVS.index(recv)],
            device_id=(depth_id, z if area_id is None else area_id),
            device_id_type=MESH,
        )

    def send(cond, args):
        waits.append((cond, args))
        copy(*args()).start()

    def received(dst, recv):
        copy(dst, dst, SENDS[0], recv, d).wait_recv()

    def block_a(b):
        return pltpu.make_async_remote_copy(
            src_ref=outa.at[b], dst_ref=ina.at[b], send_sem=snd_a.at[b], recv_sem=rcv_a.at[b],
            device_id=(d + 1, z), device_id_type=MESH,
        )

    def block_s(b):
        return pltpu.make_async_remote_copy(
            src_ref=outs.at[b], dst_ref=ins.at[b], send_sem=snd_s.at[b], recv_sem=rcv_s.at[b],
            device_id=(d - 1, z), device_id_type=MESH,
        )

    loads = [
        pltpu.make_async_copy(start_hbm, start, local.at[0]),
        pltpu.make_async_copy(inv_hbm.at[1], inv.at[1], local.at[1]),
        pltpu.make_async_copy(inv_hbm.at[0], inv.at[0], local.at[2]),
        pltpu.make_async_copy(rhs_hbm, rhs, local.at[3]),
    ]
    for load in loads:
        load.start()

    barrier = pltpu.get_barrier_semaphore()
    is_spoke = both(c % 2 == 1, c != HUB)
    partners = [
        (d > 0, d - 1, z),
        (d < depth - 1, d + 1, z),
        (z > 0, d, z - 1),
        (z < areas - 1, d, z + 1),
        (is_spoke, base + HUB, z),
        (both(c == HUB, r > 0), d - ROW, z),
        (both(c == HUB, r < rows - 1), d + ROW, z),
    ] + [(c == HUB, base + spoke, z) for spoke in SPOKES]
    for cond, to_depth, to_area in partners:

        @pl.when(cond)
        def _():
            pl.semaphore_signal(
                barrier, inc=1, device_id=(to_depth, to_area), device_id_type=MESH
            )

    kinds = facies[...]
    facies_count = lat_tab.shape[1]
    v_rows = jnp.zeros(kinds.shape, F32)
    w_rows = [jnp.zeros(kinds.shape, F32) for _ in range(lat_tab.shape[0])]
    for kind in range(facies_count):
        mask = kinds == kind
        v_rows = jnp.where(mask, vert_tab[kind], v_rows)
        w_rows = [jnp.where(mask, lat_tab[j, kind], w) for j, w in enumerate(w_rows)]
    vert[...] = v_rows
    for j, w in enumerate(w_rows):
        wts[j] = w
    wsum[...] = functools.reduce(jnp.add, w_rows)

    for t in range(tiles):
        lanes = slice(t * LANES, (t + 1) * LANES)
        for k in range(2):
            for first in (0, 2 * LANES + HW):
                lat_h[k, t, first : first + HW, :] = jnp.zeros((HW, LANES), BF16)
                lat_l[k, t, first : first + HW, :] = jnp.zeros((HW, LANES), BF16)
        for first in range(HW, 2 * LANES + HW, HW):
            place = lax.broadcasted_iota(jnp.int32, (HW, LANES), 0) + (first + t * LANES - HW)
            sums = [jnp.zeros((HW, LANES), F32) for _ in range(2)]
            for j in range(nbrs.shape[0]):
                hit = place == nbrs[j : j + 1, lanes]
                for k in range(2):
                    sums[k] = sums[k] + jnp.where(hit, wts[j, k : k + 1, lanes], 0.0)
            for k in range(2):
                high, low = split(sums[k])
                lat_h[k, t, first : first + HW, :] = high
                lat_l[k, t, first : first + HW, :] = low

    def lateral_own(k, v):
        parts = [v[:, t * LANES : (t + 1) * LANES] for t in range(tiles)]
        sums = []
        for t in range(tiles):
            first, end = max(t - 1, 0), min(t + 2, tiles)
            rows_of = slice((first - t + 1) * LANES, (end - t + 1) * LANES)
            x = jnp.concatenate(parts[first:end], axis=1)
            sums.append(dot3(x, lat_h[k, t, rows_of], lat_l[k, t, rows_of]))
        return wsum[k : k + 1, :] * v - jnp.concatenate(sums, axis=1)

    def add_neighbours(field, low, high):
        for k in range(2):
            left, right = low[...], high[...]
            if k == 1:
                left, right = pltpu.roll(left, HW, 1), pltpu.roll(right, HW, 1)
            for t, x, first in ((0, left, 0), (tiles - 1, right, 2 * LANES)):
                lanes = slice(t * LANES, (t + 1) * LANES)
                rows_of = slice(first, first + LANES)
                field[k, :, lanes] = field[k, :, lanes] + dot3(
                    x, lat_h[k, t, rows_of], lat_l[k, t, rows_of]
                )

    loads[0].wait()
    below_out[...] = vert[0:1, :] * start[0]
    partner_count = sum(cond.astype(jnp.int32) for cond, _, _ in partners)
    pl.semaphore_wait(barrier, partner_count)

    has_left, has_right = z > 0, z < areas - 1

    def halo(field, low, high, name, place):
        upper_half = lax.broadcasted_iota(jnp.int32, (count, LANES), 1) >= HW

        @pl.when(has_right)
        def _():
            edge = slice(width - LANES, width)
            to_right[place] = jnp.where(
                upper_half, field[0, :, edge], pltpu.roll(field[1, :, edge], HW, 1)
            )
            send(lambda: has_right, lambda: (
                to_right.at[place], low, name + "_right", name + "_lo", d, z + 1,
            ))

        @pl.when(has_left)
        def _():
            to_left[place] = jnp.where(
                upper_half, pltpu.roll(field[1, :, :LANES], HW, 1), field[0, :, :LANES]
            )
            send(lambda: has_left, lambda: (
                to_left.at[place], high, name + "_left", name + "_hi", d, z - 1,
            ))

        @pl.when(jnp.logical_not(has_left))
        def _():
            low[...] = jnp.zeros(low.shape, F32)

        @pl.when(jnp.logical_not(has_right))
        def _():
            high[...] = jnp.zeros(high.shape, F32)

    def halo_received(low, high, name):
        @pl.when(has_left)
        def _():
            received(low, name + "_lo")

        @pl.when(has_right)
        def _():
            received(high, name + "_hi")

    halo(start, slo, shi, "start", 0)

    @pl.when(d > 0)
    def _():
        send(lambda: d > 0, lambda: (below_out, below_in, "below", "below", d - 1))

    def split_layer(k):
        def body(i, _):
            some = pl.ds(pl.multiple_of(i * LANES, LANES), LANES)
            high, low = split(inv[k, some, :])
            dh[k, some, :] = high
            dl[k, some, :] = low
            return 0

        lax.fori_loop(0, tiles, body, 0)

    per_tile = LANES // size
    loads[1].wait()
    split_layer(1)
    loads[2].wait()

    def compose(i, _):
        some = pl.ds(pl.multiple_of(i * LANES, LANES), LANES)
        scale = jnp.transpose(jnp.broadcast_to(vert[0:1, some], (LANES, LANES)))
        left = inv[0, some, :] * vert[1:2, :] * jnp.concatenate([scale] * tiles, axis=1)
        product = dot3(left, dh[1], dl[1])
        high, low = split(product)
        th[some, :] = high
        tl[some, :] = low
        for part in range(per_tile):
            outa[i * per_tile + part] = product[part * size : (part + 1) * size]

        @pl.when(c == 0)
        def _():
            for part in range(per_tile):
                block_a(i * per_tile + part).start()

        return 0

    lax.fori_loop(0, tiles, compose, 0)

    @pl.when(c == LAST)
    def _():
        def body(i, _):
            some = pl.ds(pl.multiple_of(i * LANES, LANES), LANES)
            turned = jnp.transpose(outa[:, :, some].reshape(width, LANES))
            for part in range(per_tile):
                outs[i * per_tile + part] = turned[part * size : (part + 1) * size]
                block_s(i * per_tile + part).start()
            return 0

        lax.fori_loop(0, tiles, body, 0)

    split_layer(0)

    def own_part():
        loads[3].wait()
        g[0] = rhs[0] - lateral_own(0, start[0]) + vert[1:2, :] * start[1]
        g[1] = rhs[1] - lateral_own(1, start[1])
        halo_received(slo, shi, "start")
        add_neighbours(g, slo, shi)

        @pl.when(d < depth - 1)
        def _():
            received(below_in, "below")
            g[1] = g[1] + below_in[...]

        first = dot3(g[0], dh[0], dl[0])
        o_buf[...] = dot3(g[1] + vert[1:2, :] * first, dh[1], dl[1])

        @pl.when(c == 0)
        def _():
            f_in[...] = jnp.zeros(f_in.shape, F32)
            f_out[...] = o_buf[...]

    step_a = (c // 2) * 4 + c % 2
    last = LAST - c
    step_s = (last // 2) * 4 + last % 2
    middle = (HUB // 2) * 4 + 4 + BLOCKS - 1

    def next_f():
        return f_out, f_in, "f_next", "f", d + 1

    def row_offset():
        return f_out, o_down, "o_hub", "o", base + HUB

    def slot(s, _):
        @pl.when(both(c > 0, s >= step_a, s < step_a + BLOCKS))
        def _():
            b = s - step_a
            some = pl.ds(pl.multiple_of(b * size, size), size)
            block_a(b).wait_recv()
            high, low = split(ina[b])
            ah[some, :] = high
            al[some, :] = low

            @pl.when(c < LAST)
            def _():
                product = dot_halves(high, low, th[...], tl[...], False)
                outa[b] = product
                block_a(b).start()

                @pl.when(c == HUB)
                def _():
                    high, low = split(product)
                    bh[some, :] = high
                    bl[some, :] = low

        @pl.when(s == 1)
        def _():
            own_part()

        @pl.when(s == step_a + 1)
        def _():
            @pl.when(c > 0)
            def _():
                received(f_in, "f")
                f_out[...] = dot3(f_in[...], th[...], tl[...]) + o_buf[...]

            @pl.when(c < LAST)
            def _():
                copy(*next_f()).start()

            @pl.when(both(c == LAST, r < rows - 1))
            def _():
                copy(*row_offset()).start()

        @pl.when(both(c < LAST, s >= step_s, s < step_s + BLOCKS))
        def _():
            b = s - step_s
            some = pl.ds(pl.multiple_of(b * size, size), size)
            block_s(b).wait_recv()
            high, low = split(ins[b])
            sh[some, :] = high
            sl[some, :] = low

            @pl.when(c > 0)
            def _():
                outs[b] = dot_halves(high, low, th[...], tl[...], True)
                block_s(b).start()

        @pl.when(both(c == HUB, s > middle - tiles, s <= middle))
        def _():
            i = s - (middle - tiles + 1)
            some = pl.ds(pl.multiple_of(i * LANES, LANES), LANES)
            high, low = split(dot_halves(sh[some, :], sl[some, :], bh[...], bl[...], True))
            mh[some, :] = high
            ml[some, :] = low

        return 0

    lax.fori_loop(0, (ROW // 2 - 1) * 4 + 1 + BLOCKS, slot, 0)
    waits.append((lambda: c < LAST, next_f))
    waits.append((lambda: both(c == LAST, r < rows - 1), row_offset))

    def spread(cond, buf, name):
        @pl.when(c == HUB)
        def _():
            for spoke in SPOKES + (HUB - 1,):
                send(
                    lambda: both(cond(), c == HUB),
                    lambda spoke=spoke: (buf, buf, name + str(spoke), name, base + spoke),
                )

        @pl.when(is_spoke)
        def _():
            send(lambda: both(cond(), is_spoke), lambda: (buf, buf, name + "_pair", name, d - 1))

    @pl.when(both(c == HUB, r < rows - 1))
    def _():
        received(o_down, "o")

        @pl.when(r == 0)
        def _():
            send(
                lambda: both(c == HUB, r == 0, r < rows - 1),
                lambda: (o_down, eb, "down_hub", "down", d + ROW),
            )

    @pl.when(r == 0)
    def _():
        e_in[...] = f_in[...]

    @pl.when(r > 0)
    def _():
        received(eb, "down")
        spread(lambda: r > 0, eb, "down")

        @pl.when(both(c == HUB, r < rows - 1))
        def _():
            e_next[...] = dot3(eb[...], mh[...], ml[...], True) + o_down[...]
            send(
                lambda: both(c == HUB, r > 0, r < rows - 1),
                lambda: (e_next, eb, "down_hub", "down", d + ROW),
            )

        @pl.when(c == 0)
        def _():
            e_in[...] = eb[...]

        @pl.when(c > 0)
        def _():
            e_in[...] = dot3(eb[...], ah[...], al[...]) + f_in[...]

    entering = vert[0:1, :] * e_in[...]
    y[0] = dot3(g[0] + entering, dh[0], dl[0])
    y[1] = dot3(g[1] + vert[1:2, :] * y[0], dh[1], dl[1])
    halo(y, ylo, yhi, "y", 1)
    h[0] = rhs[0] - lateral_own(0, y[0]) + entering
    h[1] = rhs[1] - lateral_own(1, y[1]) + vert[1:2, :] * y[0]
    halo_received(ylo, yhi, "y")
    add_neighbours(h, ylo, yhi)

    def next_g():
        return g_out, g_in, "g_prev", "g", d - 1

    above = dot3(h[1], dh[1], dl[1], True)
    p_buf[...] = vert[0:1, :] * dot3(h[0] + vert[1:2, :] * above, dh[0], dl[0], True)

    @pl.when(c == LAST)
    def _():
        g_in[...] = jnp.zeros(g_in.shape, F32)
        g_out[...] = p_buf[...]
        copy(*next_g()).start()

    @pl.when(r > 0)
    def _():
        @pl.when(c == 0)
        def _():
            w_out[...] = p_buf[...]

        @pl.when(c > 0)
        def _():
            w_out[...] = dot3(p_buf[...], ah[...], al[...], True)

        @pl.when(c % 2 == 0)
        def _():
            send(
                lambda: both(r > 0, c % 2 == 0),
                lambda: (w_out, w_pair, "w_pair", "w_pair", d + 1),
            )

        @pl.when(c % 2 == 1)
        def _():
            received(w_pair, "w_pair")
            w_out[...] = w_out[...] + w_pair[...]

        for i, spoke in enumerate(SPOKES):

            @pl.when(c == spoke)
            def _():
                send(
                    lambda spoke=spoke: both(r > 0, c == spoke),
                    lambda i=i: (w_out, w_hub.at[i], "w_hub", "w" + str(i), base + HUB),
                )

        @pl.when(c == HUB)
        def _():
            for spoke in range(3):
                received(w_hub.at[spoke], "w" + str(spoke))
            o_up[...] = w_out[...] + (w_hub[0] + (w_hub[1] + w_hub[2]))

            @pl.when(r == rows - 1)
            def _():
                send(
                    lambda: both(c == HUB, r > 0, r == rows - 1),
                    lambda: (o_up, ub, "up_hub", "up", d - ROW),
                )

    @pl.when(c < LAST)
    def _():
        received(g_in, "g")

        @pl.when(c > 0)
        def _():
            g_out[...] = dot3(g_in[...], th[...], tl[...], True) + p_buf[...]
            copy(*next_g()).start()

    waits.append((lambda: c > 0, next_g))

    @pl.when(r < rows - 1)
    def _():
        received(ub, "up")
        spread(lambda: r < rows - 1, ub, "up")

        @pl.when(both(c == HUB, r > 0))
        def _():
            u_next[...] = dot3(ub[...], mh[...], ml[...]) + o_up[...]
            send(
                lambda: both(c == HUB, r > 0, r < rows - 1),
                lambda: (u_next, ub, "up_hub", "up", d - ROW),
            )

        @pl.when(c == LAST)
        def _():
            g_in[...] = ub[...]

        @pl.when(c < LAST)
        def _():
            g_in[...] = g_in[...] + dot3(ub[...], sh[...], sl[...])

    upper = dot3(h[1] + g_in[...], dh[1], dl[1], True)
    out[1] = upper
    out[0] = dot3(h[0] + vert[1:2, :] * upper, dh[0], dl[0], True)

    for cond, args in waits:
        @pl.when(cond())
        def _():
            copy(*args()).wait_send()

    @pl.when(c < LAST)
    def _():
        for b in range(BLOCKS):
            block_a(b).wait_send()

    @pl.when(c > 0)
    def _():
        for b in range(BLOCKS):
            block_s(b).wait_send()


def shards(depth, areas, rhs_field, start_field, inverses, facies, neighbours, lateral_table, vertical_table):
    layers, count, width = rhs_field.shape
    size = width // BLOCKS
    tiles = width // LANES
    field = (layers, count, width)
    matrix = (width, width)
    state = pltpu.VMEM((count, width), F32)

    def blocks():
        return pltpu.VMEM((BLOCKS, size, width), F32)

    def halves():
        return [pltpu.VMEM(matrix, BF16)] * 2

    halo = pltpu.VMEM((count, LANES), F32)
    scratch = (
        [pltpu.VMEM(field, F32)] * 2
        + [pltpu.VMEM((layers,) + matrix, F32)]
        + [pltpu.VMEM((layers,) + matrix, BF16)] * 2
        + halves()
        + [blocks()] + halves() + [blocks()]
        + [blocks()] + halves() + [blocks()]
        + halves() * 2
        + [pltpu.VMEM((layers, tiles, 3 * LANES, LANES), BF16)] * 2
        + [pltpu.VMEM((neighbours.shape[1], layers, width), F32)]
        + [pltpu.VMEM((layers, width), F32)] * 2
        + [halo] * 4
        + [pltpu.VMEM((2, count, LANES), F32)] * 2
        + [state] * 2
        + [pltpu.VMEM(field, F32)] + [state] * 4
        + [state] * 3
        + [pltpu.VMEM(field, F32)] * 2
        + [state] * 3
        + [pltpu.VMEM((3, count, width), F32)] + [state]
        + [state] * 4
        + [
            pltpu.SemaphoreType.DMA((4,)),
            pltpu.SemaphoreType.DMA((len(SENDS),)),
            pltpu.SemaphoreType.DMA((len(RECVS),)),
        ]
        + [pltpu.SemaphoreType.DMA((BLOCKS,))] * 4
    )
    vmem = pl.BlockSpec(memory_space=pltpu.VMEM)
    smem = pl.BlockSpec(memory_space=pltpu.SMEM)
    hbm = pl.BlockSpec(memory_space=pl.ANY)
    return pl.pallas_call(
        functools.partial(kernel, depth, areas),
        out_shape=jax.ShapeDtypeStruct(field, F32),
        in_specs=[smem, smem, vmem, vmem, hbm, hbm, hbm],
        out_specs=vmem,
        scratch_shapes=scratch,
        compiler_params=pltpu.CompilerParams(
            collective_id=0, has_side_effects=True, vmem_limit_bytes=60 * 1024 * 1024
        ),
        name="sweep",
    )(lateral_table.T, vertical_table, facies, neighbours.T, rhs_field, start_field, inverses)


def solution(mesh):
    return jax.shard_map(
        functools.partial(shards, mesh.shape["depth"], mesh.shape["area"]),
        mesh=mesh,
        in_specs=(
            P("depth", None, "area"),
            P("depth", None, "area"),
            P("depth", "area", None),
            P("depth", "area"),
            P("area", None),
            P(),
            P(),
        ),
        out_specs=P("depth", None, "area"),
        check_vma=False,
    )
```

```python
import functools

import jax
import jax.numpy as jnp
from jax import lax
from jax.experimental import pallas as pl
from jax.experimental.pallas import tpu as pltpu
from jax.sharding import PartitionSpec as P

MESH = pl.DeviceIdType.MESH
F32 = jnp.float32
BF16 = jnp.bfloat16
HW = 64
LANES = 128
ROW = 8
LAST = ROW - 1
HUB = 3
SPOKES = (7, 1, 5)
BLOCKS = 8

SENDS = (
    "start_right", "start_left", "below", "f_next", "o_hub", "down_hub",
    "down_far", "down1", "down5", "down2", "down_pair", "y_right",
    "y_left", "w_pair", "w_hub", "g_prev", "up_hub", "up_far",
    "up1", "up5", "up2", "up_pair",
)
RECVS = (
    "start_lo", "start_hi", "below", "f", "o", "down",
    "y_lo", "y_hi", "w_pair", "w0", "w1", "w2",
    "g", "up",
)


def split(x):
    high = x.astype(BF16)
    return high, (x - high.astype(F32)).astype(BF16)


def dot3(x, w_high, w_low, transposed=False):
    return dot_halves(*split(x), w_high, w_low, transposed)


def dot_halves(high, low, w_high, w_low, transposed):
    dims = (((1,), (1 if transposed else 0,)), ((), ()))
    rows = high.shape[0]
    both = lax.dot_general(
        jnp.concatenate([high, low], axis=0), w_high, dims, preferred_element_type=F32
    )
    rest = lax.dot_general(high, w_low, dims, preferred_element_type=F32)
    return both[:rows] + both[rows:] + rest


def kernel(
    depth, areas,
    lat_tab, vert_tab, facies, nbrs, rhs_hbm, start_hbm, inv_hbm,
    out,
    rhs, start, inv, dh, dl, dth, dtl, th, tl, tth, ttl, ina, ah, al, outa, ins, sh, sl, outs, bh, bl, mh, ml,
    lat_h, lat_l, wts, wsum, vert, slo, shi, ylo, yhi, to_right, to_left, below_out, below_in,
    g, f_in, f_out, o_buf, o_down, eb, e_next, e_in, y, h, p_buf, w_out, w_pair, w_hub, o_up,
    g_in, g_out, ub, u_next,
    local, snd, rcv, snd_a, rcv_a, snd_s, rcv_s,
):
    rows = depth // ROW
    d = lax.axis_index("depth")
    z = lax.axis_index("area")
    r, c = d // ROW, d % ROW
    width = out.shape[2]
    count = out.shape[1]
    tiles = width // LANES
    size = width // BLOCKS
    base = r * ROW
    waits = []

    def both(*conds):
        return functools.reduce(jnp.logical_and, conds)

    def copy(src, dst, send, recv, depth_id, area_id=None):
        return pltpu.make_async_remote_copy(
            src_ref=src,
            dst_ref=dst,
            send_sem=snd.at[SENDS.index(send)],
            recv_sem=rcv.at[RECVS.index(recv)],
            device_id=(depth_id, z if area_id is None else area_id),
            device_id_type=MESH,
        )

    def send(cond, args):
        waits.append((cond, args))
        copy(*args()).start()

    def received(dst, recv):
        copy(dst, dst, SENDS[0], recv, d).wait_recv()

    def block_a(b):
        return pltpu.make_async_remote_copy(
            src_ref=outa.at[b], dst_ref=ina.at[b], send_sem=snd_a.at[b], recv_sem=rcv_a.at[b],
            device_id=(d + 1, z), device_id_type=MESH,
        )

    def block_s(b):
        return pltpu.make_async_remote_copy(
            src_ref=outs.at[b], dst_ref=ins.at[b], send_sem=snd_s.at[b], recv_sem=rcv_s.at[b],
            device_id=(d - 1, z), device_id_type=MESH,
        )

    loads = [
        pltpu.make_async_copy(start_hbm, start, local.at[0]),
        pltpu.make_async_copy(inv_hbm.at[1], inv.at[1], local.at[1]),
        pltpu.make_async_copy(inv_hbm.at[0], inv.at[0], local.at[2]),
        pltpu.make_async_copy(rhs_hbm, rhs, local.at[3]),
    ]
    for load in loads:
        load.start()

    barrier = pltpu.get_barrier_semaphore()
    is_spoke = both(c % 2 == 1, c != HUB)
    partners = [
        (d > 0, d - 1, z),
        (d < depth - 1, d + 1, z),
        (z > 0, d, z - 1),
        (z < areas - 1, d, z + 1),
        (is_spoke, base + HUB, z),
        (both(c == HUB, r > 0), d - ROW, z),
        (both(c == HUB, r < rows - 1), d + ROW, z),
        (both(c == HUB, r > 0), d - ROW + (LAST - HUB), z),
        (both(c == HUB, r < rows - 1), d + ROW + (LAST - HUB), z),
        (both(c == LAST, r > 0), d - ROW - (LAST - HUB), z),
        (both(c == LAST, r < rows - 1), d + ROW - (LAST - HUB), z),
        (both(c == LAST, r == 0, r < rows - 1), d + ROW, z),
        (both(c == LAST, r == 1), d - ROW, z),
    ] + [(c == HUB, base + spoke, z) for spoke in SPOKES]
    for cond, to_depth, to_area in partners:

        @pl.when(cond)
        def _():
            pl.semaphore_signal(
                barrier, inc=1, device_id=(to_depth, to_area), device_id_type=MESH
            )

    kinds = facies[...]
    facies_count = lat_tab.shape[1]
    v_rows = jnp.zeros(kinds.shape, F32)
    w_rows = [jnp.zeros(kinds.shape, F32) for _ in range(lat_tab.shape[0])]
    for kind in range(facies_count):
        mask = kinds == kind
        v_rows = jnp.where(mask, vert_tab[kind], v_rows)
        w_rows = [jnp.where(mask, lat_tab[j, kind], w) for j, w in enumerate(w_rows)]
    vert[...] = v_rows
    for j, w in enumerate(w_rows):
        wts[j] = w
    wsum[...] = functools.reduce(jnp.add, w_rows)

    for t in range(tiles):
        lanes = slice(t * LANES, (t + 1) * LANES)
        for k in range(2):
            for first in (0, 2 * LANES + HW):
                lat_h[k, t, first : first + HW, :] = jnp.zeros((HW, LANES), BF16)
                lat_l[k, t, first : first + HW, :] = jnp.zeros((HW, LANES), BF16)
        for first in range(HW, 2 * LANES + HW, HW):
            place = lax.broadcasted_iota(jnp.int32, (HW, LANES), 0) + (first + t * LANES - HW)
            sums = [jnp.zeros((HW, LANES), F32) for _ in range(2)]
            for j in range(nbrs.shape[0]):
                hit = place == nbrs[j : j + 1, lanes]
                for k in range(2):
                    sums[k] = sums[k] + jnp.where(hit, wts[j, k : k + 1, lanes], 0.0)
            for k in range(2):
                high, low = split(sums[k])
                lat_h[k, t, first : first + HW, :] = high
                lat_l[k, t, first : first + HW, :] = low

    def lateral_own(k, v):
        parts = [v[:, t * LANES : (t + 1) * LANES] for t in range(tiles)]
        sums = []
        for t in range(tiles):
            first, end = max(t - 1, 0), min(t + 2, tiles)
            rows_of = slice((first - t + 1) * LANES, (end - t + 1) * LANES)
            x = jnp.concatenate(parts[first:end], axis=1)
            sums.append(dot3(x, lat_h[k, t, rows_of], lat_l[k, t, rows_of]))
        return wsum[k : k + 1, :] * v - jnp.concatenate(sums, axis=1)

    def add_neighbours(field, low, high):
        for k in range(2):
            left, right = low[...], high[...]
            if k == 1:
                left, right = pltpu.roll(left, HW, 1), pltpu.roll(right, HW, 1)
            for t, x, first in ((0, left, 0), (tiles - 1, right, 2 * LANES)):
                lanes = slice(t * LANES, (t + 1) * LANES)
                rows_of = slice(first, first + LANES)
                field[k, :, lanes] = field[k, :, lanes] + dot3(
                    x, lat_h[k, t, rows_of], lat_l[k, t, rows_of]
                )

    loads[0].wait()
    below_out[...] = vert[0:1, :] * start[0]
    partner_count = sum(cond.astype(jnp.int32) for cond, _, _ in partners)
    pl.semaphore_wait(barrier, partner_count)

    has_left, has_right = z > 0, z < areas - 1

    def halo(field, low, high, name, place):
        upper_half = lax.broadcasted_iota(jnp.int32, (count, LANES), 1) >= HW

        @pl.when(has_right)
        def _():
            edge = slice(width - LANES, width)
            to_right[place] = jnp.where(
                upper_half, field[0, :, edge], pltpu.roll(field[1, :, edge], HW, 1)
            )
            send(lambda: has_right, lambda: (
                to_right.at[place], low, name + "_right", name + "_lo", d, z + 1,
            ))

        @pl.when(has_left)
        def _():
            to_left[place] = jnp.where(
                upper_half, pltpu.roll(field[1, :, :LANES], HW, 1), field[0, :, :LANES]
            )
            send(lambda: has_left, lambda: (
                to_left.at[place], high, name + "_left", name + "_hi", d, z - 1,
            ))

        @pl.when(jnp.logical_not(has_left))
        def _():
            low[...] = jnp.zeros(low.shape, F32)

        @pl.when(jnp.logical_not(has_right))
        def _():
            high[...] = jnp.zeros(high.shape, F32)

    def halo_received(low, high, name):
        @pl.when(has_left)
        def _():
            received(low, name + "_lo")

        @pl.when(has_right)
        def _():
            received(high, name + "_hi")

    halo(start, slo, shi, "start", 0)

    @pl.when(d > 0)
    def _():
        send(lambda: d > 0, lambda: (below_out, below_in, "below", "below", d - 1))

    def split_layer(k):
        def body(i, _):
            some = pl.ds(pl.multiple_of(i * LANES, LANES), LANES)
            high, low = split(inv[k, some, :])
            dh[k, some, :] = high
            dl[k, some, :] = low
            return 0

        lax.fori_loop(0, tiles, body, 0)

    per_tile = LANES // size
    loads[1].wait()
    split_layer(1)
    loads[2].wait()

    def compose(i, _):
        some = pl.ds(pl.multiple_of(i * LANES, LANES), LANES)
        scale = jnp.transpose(jnp.broadcast_to(vert[0:1, some], (LANES, LANES)))
        left = inv[0, some, :] * vert[1:2, :] * jnp.concatenate([scale] * tiles, axis=1)
        product = dot3(left, dh[1], dl[1])
        high, low = split(product)
        th[some, :] = high
        tl[some, :] = low
        for part in range(per_tile):
            outa[i * per_tile + part] = product[part * size : (part + 1) * size]
        turned = jnp.transpose(product)
        outs[:, :, some] = turned.reshape(BLOCKS, size, LANES)
        high, low = split(turned)
        tth[:, some] = high
        ttl[:, some] = low

        @pl.when(c == 0)
        def _():
            for part in range(per_tile):
                block_a(i * per_tile + part).start()

        return 0

    lax.fori_loop(0, tiles, compose, 0)

    @pl.when(c == LAST)
    def _():
        for b in range(BLOCKS):
            block_s(b).start()

    split_layer(0)

    def own_part():
        loads[3].wait()
        g[0] = rhs[0] - lateral_own(0, start[0]) + vert[1:2, :] * start[1]
        g[1] = rhs[1] - lateral_own(1, start[1])
        halo_received(slo, shi, "start")
        add_neighbours(g, slo, shi)

        @pl.when(d < depth - 1)
        def _():
            received(below_in, "below")
            g[1] = g[1] + below_in[...]

        first = dot3(g[0], dh[0], dl[0])
        o_buf[...] = dot3(g[1] + vert[1:2, :] * first, dh[1], dl[1])

        @pl.when(c == 0)
        def _():
            f_in[...] = jnp.zeros(f_in.shape, F32)
            f_out[...] = o_buf[...]

    step_a = (c // 2) * 4 + c % 2
    last = LAST - c
    step_s = (last // 2) * 4 + last % 2
    middle = (HUB // 2) * 4 + 4 + BLOCKS - 1

    def next_f():
        return f_out, f_in, "f_next", "f", d + 1

    def row_offset():
        return f_out, o_down, "o_hub", "o", base + HUB

    def first_offset():
        return f_out, eb, "down_hub", "down", base + ROW + HUB

    def first_far():
        return f_out, eb, "down_far", "down", base + ROW + LAST

    step_f = jnp.maximum(step_a + 1, 2)

    def slot(s, _):
        @pl.when(both(c > 0, s >= step_a, s < step_a + BLOCKS))
        def _():
            b = s - step_a
            some = pl.ds(pl.multiple_of(b * size, size), size)
            block_a(b).wait_recv()
            high, low = split(ina[b])
            ah[some, :] = high
            al[some, :] = low

            @pl.when(c < LAST)
            def _():
                product = dot_halves(high, low, th[...], tl[...], False)
                outa[b] = product
                block_a(b).start()

                @pl.when(c == HUB)
                def _():
                    high, low = split(product)
                    bh[some, :] = high
                    bl[some, :] = low

        @pl.when(both(c < LAST, s >= step_s, s < step_s + BLOCKS))
        def _():
            b = s - step_s
            some = pl.ds(pl.multiple_of(b * size, size), size)
            block_s(b).wait_recv()
            high, low = split(ins[b])
            sh[some, :] = high
            sl[some, :] = low

            @pl.when(c > 0)
            def _():
                outs[b] = dot_halves(high, low, tth[...], ttl[...], False)
                block_s(b).start()

        @pl.when(s == 2)
        def _():
            own_part()

        @pl.when(s == step_f)
        def _():
            @pl.when(c > 0)
            def _():
                received(f_in, "f")
                f_out[...] = dot3(f_in[...], th[...], tl[...]) + o_buf[...]

            @pl.when(c < LAST)
            def _():
                copy(*next_f()).start()

            @pl.when(both(c == LAST, r > 0, r < rows - 1))
            def _():
                copy(*row_offset()).start()

            @pl.when(both(c == LAST, r == 0, r < rows - 1))
            def _():
                copy(*first_offset()).start()
                copy(*first_far()).start()

        @pl.when(both(s > 2, s < 5))
        def _():
            k = s - 3
            for t in range(tiles):
                lanes = slice(t * LANES, (t + 1) * LANES)
                dth[k, :, lanes] = jnp.transpose(dh[k, lanes, :])
                dtl[k, :, lanes] = jnp.transpose(dl[k, lanes, :])

        @pl.when(both(c == HUB, s > middle - tiles, s <= middle))
        def _():
            i = s - (middle - tiles + 1)
            some = pl.ds(pl.multiple_of(i * LANES, LANES), LANES)
            high, low = split(dot_halves(sh[some, :], sl[some, :], bh[...], bl[...], True))
            mh[some, :] = high
            ml[some, :] = low

        return 0

    lax.fori_loop(0, (ROW // 2 - 1) * 4 + 1 + BLOCKS, slot, 0)
    waits.append((lambda: c < LAST, next_f))
    waits.append((lambda: both(c == LAST, r > 0, r < rows - 1), row_offset))
    waits.append((lambda: both(c == LAST, r == 0, r < rows - 1), first_offset))
    waits.append((lambda: both(c == LAST, r == 0, r < rows - 1), first_far))

    def spread(cond, buf, name):
        @pl.when(c == HUB)
        def _():
            for spoke in (1, 5, HUB - 1):
                send(
                    lambda: both(cond(), c == HUB),
                    lambda spoke=spoke: (buf, buf, name + str(spoke), name, base + spoke),
                )

        @pl.when(is_spoke)
        def _():
            send(lambda: both(cond(), is_spoke), lambda: (buf, buf, name + "_pair", name, d - 1))

    @pl.when(r == 0)
    def _():
        e_in[...] = f_in[...]

    @pl.when(r > 0)
    def _():
        received(eb, "down")
        spread(lambda: r > 0, eb, "down")

        @pl.when(both(c == HUB, r < rows - 1))
        def _():
            received(o_down, "o")
            e_next[...] = dot3(eb[...], mh[...], ml[...], True) + o_down[...]
            for name, to in (("down_hub", HUB), ("down_far", LAST)):
                send(
                    lambda: both(c == HUB, r > 0, r < rows - 1),
                    lambda name=name, to=to: (e_next, eb, name, "down", base + ROW + to),
                )

        @pl.when(c == 0)
        def _():
            e_in[...] = eb[...]

        @pl.when(c > 0)
        def _():
            e_in[...] = dot3(eb[...], ah[...], al[...]) + f_in[...]

    entering = vert[0:1, :] * e_in[...]
    y[0] = dot3(g[0] + entering, dh[0], dl[0])
    y[1] = dot3(g[1] + vert[1:2, :] * y[0], dh[1], dl[1])
    halo(y, ylo, yhi, "y", 1)
    h[0] = rhs[0] - lateral_own(0, y[0]) + entering
    h[1] = rhs[1] - lateral_own(1, y[1]) + vert[1:2, :] * y[0]
    halo_received(ylo, yhi, "y")
    add_neighbours(h, ylo, yhi)

    def next_g():
        return g_out, g_in, "g_prev", "g", d - 1

    above = dot3(h[1], dth[1], dtl[1])
    p_buf[...] = vert[0:1, :] * dot3(h[0] + vert[1:2, :] * above, dth[0], dtl[0])

    @pl.when(c == LAST)
    def _():
        g_in[...] = jnp.zeros(g_in.shape, F32)
        g_out[...] = p_buf[...]
        copy(*next_g()).start()

    @pl.when(r > 0)
    def _():
        @pl.when(c == 0)
        def _():
            w_out[...] = p_buf[...]

        @pl.when(c > 0)
        def _():
            w_out[...] = dot3(p_buf[...], ah[...], al[...], True)

        @pl.when(c % 2 == 0)
        def _():
            send(
                lambda: both(r > 0, c % 2 == 0),
                lambda: (w_out, w_pair, "w_pair", "w_pair", d + 1),
            )

        @pl.when(c % 2 == 1)
        def _():
            received(w_pair, "w_pair")
            w_out[...] = w_out[...] + w_pair[...]

        for i, spoke in enumerate(SPOKES):

            @pl.when(c == spoke)
            def _():
                send(
                    lambda spoke=spoke: both(r > 0, c == spoke),
                    lambda i=i: (w_out, w_hub.at[i], "w_hub", "w" + str(i), base + HUB),
                )

        @pl.when(c == HUB)
        def _():
            for spoke in range(3):
                received(w_hub.at[spoke], "w" + str(spoke))
            o_up[...] = w_out[...] + (w_hub[0] + (w_hub[1] + w_hub[2]))

            @pl.when(r == rows - 1)
            def _():
                for name, to in (("up_hub", HUB), ("up_far", LAST)):
                    send(
                        lambda: both(c == HUB, r > 0, r == rows - 1),
                        lambda name=name, to=to: (o_up, ub, name, "up", base - ROW + to),
                    )

    @pl.when(c < LAST)
    def _():
        received(g_in, "g")

        @pl.when(c > 0)
        def _():
            g_out[...] = dot3(g_in[...], tth[...], ttl[...]) + p_buf[...]
            copy(*next_g()).start()

    waits.append((lambda: c > 0, next_g))

    @pl.when(r < rows - 1)
    def _():
        received(ub, "up")
        spread(lambda: r < rows - 1, ub, "up")

        @pl.when(both(c == HUB, r > 0))
        def _():
            u_next[...] = dot3(ub[...], mh[...], ml[...]) + o_up[...]
            for name, to in (("up_hub", HUB), ("up_far", LAST)):
                send(
                    lambda: both(c == HUB, r > 0, r < rows - 1),
                    lambda name=name, to=to: (u_next, ub, name, "up", base - ROW + to),
                )

        @pl.when(c == LAST)
        def _():
            g_in[...] = ub[...]

        @pl.when(c < LAST)
        def _():
            g_in[...] = g_in[...] + dot3(ub[...], sh[...], sl[...])

    upper = dot3(h[1] + g_in[...], dth[1], dtl[1])
    out[1] = upper
    out[0] = dot3(h[0] + vert[1:2, :] * upper, dth[0], dtl[0])

    for cond, args in waits:
        @pl.when(cond())
        def _():
            copy(*args()).wait_send()

    @pl.when(c < LAST)
    def _():
        for b in range(BLOCKS):
            block_a(b).wait_send()

    @pl.when(c > 0)
    def _():
        for b in range(BLOCKS):
            block_s(b).wait_send()


def shards(depth, areas, rhs_field, start_field, inverses, facies, neighbours, lateral_table, vertical_table):
    layers, count, width = rhs_field.shape
    size = width // BLOCKS
    tiles = width // LANES
    field = (layers, count, width)
    matrix = (width, width)
    state = pltpu.VMEM((count, width), F32)

    def blocks():
        return pltpu.VMEM((BLOCKS, size, width), F32)

    def halves():
        return [pltpu.VMEM(matrix, BF16)] * 2

    halo = pltpu.VMEM((count, LANES), F32)
    scratch = (
        [pltpu.VMEM(field, F32)] * 2
        + [pltpu.VMEM((layers,) + matrix, F32)]
        + [pltpu.VMEM((layers,) + matrix, BF16)] * 4
        + halves() * 2
        + [blocks()] + halves() + [blocks()]
        + [blocks()] + halves() + [blocks()]
        + halves() * 2
        + [pltpu.VMEM((layers, tiles, 3 * LANES, LANES), BF16)] * 2
        + [pltpu.VMEM((neighbours.shape[1], layers, width), F32)]
        + [pltpu.VMEM((layers, width), F32)] * 2
        + [halo] * 4
        + [pltpu.VMEM((2, count, LANES), F32)] * 2
        + [state] * 2
        + [pltpu.VMEM(field, F32)] + [state] * 4
        + [state] * 3
        + [pltpu.VMEM(field, F32)] * 2
        + [state] * 3
        + [pltpu.VMEM((3, count, width), F32)] + [state]
        + [state] * 4
        + [
            pltpu.SemaphoreType.DMA((4,)),
            pltpu.SemaphoreType.DMA((len(SENDS),)),
            pltpu.SemaphoreType.DMA((len(RECVS),)),
        ]
        + [pltpu.SemaphoreType.DMA((BLOCKS,))] * 4
    )
    vmem = pl.BlockSpec(memory_space=pltpu.VMEM)
    smem = pl.BlockSpec(memory_space=pltpu.SMEM)
    hbm = pl.BlockSpec(memory_space=pl.ANY)
    return pl.pallas_call(
        functools.partial(kernel, depth, areas),
        out_shape=pltpu.VMEM(field, F32),
        in_specs=[smem, smem, vmem, vmem, hbm, hbm, hbm],
        out_specs=vmem,
        scratch_shapes=scratch,
        compiler_params=pltpu.CompilerParams(
            collective_id=0, has_side_effects=True, vmem_limit_bytes=60 * 1024 * 1024
        ),
        name="sweep",
    )(lateral_table.T, vertical_table, facies, neighbours.T, rhs_field, start_field, inverses)


def solution(mesh):
    return jax.shard_map(
        functools.partial(shards, mesh.shape["depth"], mesh.shape["area"]),
        mesh=mesh,
        in_specs=(
            P("depth", None, "area"),
            P("depth", None, "area"),
            P("depth", "area", None),
            P("depth", "area"),
            P("area", None),
            P(),
            P(),
        ),
        out_specs=P("depth", None, "area"),
        check_vma=False,
    )
```

```python
import functools

import jax
import jax.numpy as jnp
from jax import lax
from jax.experimental import pallas as pl
from jax.experimental.pallas import tpu as pltpu
from jax.sharding import PartitionSpec as P

MESH = pl.DeviceIdType.MESH
F32 = jnp.float32
BF16 = jnp.bfloat16
HW = 64
LANES = 128
ROW = 8
LAST = ROW - 1
HUB = 3
SPOKES = (7, 1, 5)
OUTER = (6, 0, 4)
BLOCKS = 8

SENDS = (
    "start_right", "start_left", "below", "f_next", "o_hub", "down_hub",
    "down_far", "down1", "down5", "down2", "down_pair", "y_right",
    "y_left", "w_pair", "w_hub", "g_prev", "up_hub", "up_far",
    "up1", "up5", "up2", "up_pair",
)
RECVS = (
    "start_lo", "start_hi", "below", "f", "o", "down",
    "y_lo", "y_hi", "w_pair", "w0", "w1", "w2",
    "w3", "w4", "w5", "g", "up",
)


def split(x):
    high = x.astype(BF16)
    return high, (x - high.astype(F32)).astype(BF16)


def dot3(x, w_high, w_low, transposed=False):
    return dot_halves(*split(x), w_high, w_low, transposed)


def dot_halves(high, low, w_high, w_low, transposed):
    dims = (((1,), (1 if transposed else 0,)), ((), ()))
    rows = high.shape[0]
    both = lax.dot_general(
        jnp.concatenate([high, low], axis=0), w_high, dims, preferred_element_type=F32
    )
    rest = lax.dot_general(high, w_low, dims, preferred_element_type=F32)
    return both[:rows] + both[rows:] + rest


def kernel(
    depth, areas,
    lat_tab, vert_tab, facies, nbrs, rhs_hbm, start_hbm, inv_hbm,
    out,
    rhs, start, inv, dh, dl, dth, dtl, th, tl, tth, ttl, ina, ah, al, outa, ins, sh, sl, outs, bh, bl, mh, ml,
    lat_h, lat_l, wts, wsum, vert, slo, shi, ylo, yhi, to_right, to_left, below_out, below_in,
    g, f_in, f_out, o_buf, o_down, eb, e_next, e_in, y, h, p_buf, w_out, w_pair, w_hub, o_up,
    g_in, g_out, ub, u_next,
    local, snd, rcv, snd_a, rcv_a, snd_s, rcv_s,
):
    rows = depth // ROW
    d = lax.axis_index("depth")
    z = lax.axis_index("area")
    r, c = d // ROW, d % ROW
    width = out.shape[2]
    count = out.shape[1]
    tiles = width // LANES
    size = width // BLOCKS
    base = r * ROW
    has_a = r > 0
    has_s = r < rows - 1
    waits = []

    def both(*conds):
        return functools.reduce(jnp.logical_and, conds)

    def half(part):
        return pl.ds(part * (count // 2), count // 2)

    def copy(src, dst, send, recv, depth_id, area_id=None, part=None):
        if part is not None:
            src, dst = src.at[half(part)], dst.at[half(part)]
        return pltpu.make_async_remote_copy(
            src_ref=src,
            dst_ref=dst,
            send_sem=snd.at[SENDS.index(send), part or 0],
            recv_sem=rcv.at[RECVS.index(recv), part or 0],
            device_id=(depth_id, z if area_id is None else area_id),
            device_id_type=MESH,
        )

    def send(cond, args):
        waits.append((cond, args))
        copy(*args()).start()

    def received(dst, recv, part=None):
        copy(dst, dst, SENDS[0], recv, d, None, part).wait_recv()

    def block_a(b):
        return pltpu.make_async_remote_copy(
            src_ref=outa.at[b], dst_ref=ina.at[b], send_sem=snd_a.at[b], recv_sem=rcv_a.at[b],
            device_id=(d + 1, z), device_id_type=MESH,
        )

    def block_s(b):
        return pltpu.make_async_remote_copy(
            src_ref=outs.at[b], dst_ref=ins.at[b], send_sem=snd_s.at[b], recv_sem=rcv_s.at[b],
            device_id=(d - 1, z), device_id_type=MESH,
        )

    loads = [
        pltpu.make_async_copy(start_hbm, start, local.at[0]),
        pltpu.make_async_copy(inv_hbm.at[1], inv.at[1], local.at[1]),
        pltpu.make_async_copy(inv_hbm.at[0], inv.at[0], local.at[2]),
        pltpu.make_async_copy(rhs_hbm, rhs, local.at[3]),
    ]
    for load in loads:
        load.start()

    barrier = pltpu.get_barrier_semaphore()
    is_spoke = both(c % 2 == 1, c != HUB)
    partners = [
        (d > 0, d - 1, z),
        (d < depth - 1, d + 1, z),
        (z > 0, d, z - 1),
        (z < areas - 1, d, z + 1),
        (is_spoke, base + HUB, z),
        (both(c == HUB, r > 0), d - ROW, z),
        (both(c == HUB, r < rows - 1), d + ROW, z),
        (both(c == HUB, r > 0), d - ROW + (LAST - HUB), z),
        (both(c == HUB, r < rows - 1), d + ROW + (LAST - HUB), z),
        (both(c == LAST, r > 0), d - ROW - (LAST - HUB), z),
        (both(c == LAST, r < rows - 1), d + ROW - (LAST - HUB), z),
        (both(c == LAST, r == 0, r < rows - 1), d + ROW, z),
        (both(c == LAST, r == 1), d - ROW, z),
        (both(c % 2 == 0, c != HUB - 1), base + HUB, z),
    ] + [(c == HUB, base + other, z) for other in SPOKES + OUTER]
    for cond, to_depth, to_area in partners:

        @pl.when(cond)
        def _():
            pl.semaphore_signal(
                barrier, inc=1, device_id=(to_depth, to_area), device_id_type=MESH
            )

    kinds = facies[...]
    facies_count = lat_tab.shape[1]
    v_rows = jnp.zeros(kinds.shape, F32)
    w_rows = [jnp.zeros(kinds.shape, F32) for _ in range(lat_tab.shape[0])]
    for kind in range(facies_count):
        mask = kinds == kind
        v_rows = jnp.where(mask, vert_tab[kind], v_rows)
        w_rows = [jnp.where(mask, lat_tab[j, kind], w) for j, w in enumerate(w_rows)]
    vert[...] = v_rows
    for j, w in enumerate(w_rows):
        wts[j] = w
    wsum[...] = functools.reduce(jnp.add, w_rows)

    for t in range(tiles):
        lanes = slice(t * LANES, (t + 1) * LANES)
        for k in range(2):
            for first in (0, 2 * LANES + HW):
                lat_h[k, t, first : first + HW, :] = jnp.zeros((HW, LANES), BF16)
                lat_l[k, t, first : first + HW, :] = jnp.zeros((HW, LANES), BF16)
        for first in range(HW, 2 * LANES + HW, HW):
            place = lax.broadcasted_iota(jnp.int32, (HW, LANES), 0) + (first + t * LANES - HW)
            sums = [jnp.zeros((HW, LANES), F32) for _ in range(2)]
            for j in range(nbrs.shape[0]):
                hit = place == nbrs[j : j + 1, lanes]
                for k in range(2):
                    sums[k] = sums[k] + jnp.where(hit, wts[j, k : k + 1, lanes], 0.0)
            for k in range(2):
                high, low = split(sums[k])
                lat_h[k, t, first : first + HW, :] = high
                lat_l[k, t, first : first + HW, :] = low

    def lateral_own(k, v):
        parts = [v[:, t * LANES : (t + 1) * LANES] for t in range(tiles)]
        sums = []
        for t in range(tiles):
            first, end = max(t - 1, 0), min(t + 2, tiles)
            rows_of = slice((first - t + 1) * LANES, (end - t + 1) * LANES)
            x = jnp.concatenate(parts[first:end], axis=1)
            sums.append(dot3(x, lat_h[k, t, rows_of], lat_l[k, t, rows_of]))
        return wsum[k : k + 1, :] * v - jnp.concatenate(sums, axis=1)

    def add_neighbours(field, low, high):
        for k in range(2):
            left, right = low[...], high[...]
            if k == 1:
                left, right = pltpu.roll(left, HW, 1), pltpu.roll(right, HW, 1)
            for t, x, first in ((0, left, 0), (tiles - 1, right, 2 * LANES)):
                lanes = slice(t * LANES, (t + 1) * LANES)
                rows_of = slice(first, first + LANES)
                field[k, :, lanes] = field[k, :, lanes] + dot3(
                    x, lat_h[k, t, rows_of], lat_l[k, t, rows_of]
                )

    loads[0].wait()
    below_out[...] = vert[0:1, :] * start[0]
    partner_count = sum(cond.astype(jnp.int32) for cond, _, _ in partners)
    pl.semaphore_wait(barrier, partner_count)

    has_left, has_right = z > 0, z < areas - 1

    def halo(field, low, high, name, place):
        upper_half = lax.broadcasted_iota(jnp.int32, (count, LANES), 1) >= HW

        @pl.when(has_right)
        def _():
            edge = slice(width - LANES, width)
            to_right[place] = jnp.where(
                upper_half, field[0, :, edge], pltpu.roll(field[1, :, edge], HW, 1)
            )
            send(lambda: has_right, lambda: (
                to_right.at[place], low, name + "_right", name + "_lo", d, z + 1,
            ))

        @pl.when(has_left)
        def _():
            to_left[place] = jnp.where(
                upper_half, pltpu.roll(field[1, :, :LANES], HW, 1), field[0, :, :LANES]
            )
            send(lambda: has_left, lambda: (
                to_left.at[place], high, name + "_left", name + "_hi", d, z - 1,
            ))

        @pl.when(jnp.logical_not(has_left))
        def _():
            low[...] = jnp.zeros(low.shape, F32)

        @pl.when(jnp.logical_not(has_right))
        def _():
            high[...] = jnp.zeros(high.shape, F32)

    def halo_received(low, high, name):
        @pl.when(has_left)
        def _():
            received(low, name + "_lo")

        @pl.when(has_right)
        def _():
            received(high, name + "_hi")

    halo(start, slo, shi, "start", 0)

    @pl.when(d > 0)
    def _():
        send(lambda: d > 0, lambda: (below_out, below_in, "below", "below", d - 1))

    def split_layer(k):
        def body(i, _):
            some = pl.ds(pl.multiple_of(i * LANES, LANES), LANES)
            high, low = split(inv[k, some, :])
            dh[k, some, :] = high
            dl[k, some, :] = low
            return 0

        lax.fori_loop(0, tiles, body, 0)

    per_tile = LANES // size

    def scaled_rows(some):
        scale = jnp.transpose(jnp.broadcast_to(vert[0:1, some], (LANES, LANES)))
        return inv[0, some, :] * vert[1:2, :] * jnp.concatenate([scale] * tiles, axis=1)

    def compose(i, _):
        some = pl.ds(pl.multiple_of(i * LANES, LANES), LANES)
        product = dot3(scaled_rows(some), dh[1], dl[1])
        high, low = split(product)
        th[some, :] = high
        tl[some, :] = low
        for part in range(per_tile):
            outa[i * per_tile + part] = product[part * size : (part + 1) * size]

        @pl.when(both(c == 0, has_a))
        def _():
            for part in range(per_tile):
                block_a(i * per_tile + part).start()

        return 0

    def turn(i, _):
        some = pl.ds(pl.multiple_of(i * LANES, LANES), LANES)
        tth[:, some] = jnp.transpose(th[some, :])
        ttl[:, some] = jnp.transpose(tl[some, :])
        return 0

    def halves_of_left(i, _):
        some = pl.ds(pl.multiple_of(i * LANES, LANES), LANES)
        high, low = split(scaled_rows(some))
        sh[some, :] = high
        sl[some, :] = low
        return 0

    def compose_turned(i, _):
        some = pl.ds(pl.multiple_of(i * LANES, LANES), LANES)
        product = dot3(jnp.transpose(inv[1, :, some]), sh[...], sl[...], True)
        for part in range(per_tile):
            outs[i * per_tile + part] = product[part * size : (part + 1) * size]
            block_s(i * per_tile + part).start()
        high, low = split(product)
        tth[some, :] = high
        ttl[some, :] = low
        th[:, some] = jnp.transpose(high)
        tl[:, some] = jnp.transpose(low)
        return 0

    starts_s = both(c == LAST, has_s)
    loads[1].wait()
    loads[2].wait()

    @pl.when(starts_s)
    def _():
        lax.fori_loop(0, tiles, halves_of_left, 0)
        lax.fori_loop(0, tiles, compose_turned, 0)
        split_layer(1)

    @pl.when(jnp.logical_not(starts_s))
    def _():
        split_layer(1)
        lax.fori_loop(0, tiles, compose, 0)
        lax.fori_loop(0, tiles, turn, 0)

    split_layer(0)

    def own_part():
        loads[3].wait()
        g[0] = rhs[0] - lateral_own(0, start[0]) + vert[1:2, :] * start[1]
        g[1] = rhs[1] - lateral_own(1, start[1])
        halo_received(slo, shi, "start")
        add_neighbours(g, slo, shi)

        @pl.when(d < depth - 1)
        def _():
            received(below_in, "below")
            g[1] = g[1] + below_in[...]

        first = dot3(g[0], dh[0], dl[0])
        o_buf[...] = dot3(g[1] + vert[1:2, :] * first, dh[1], dl[1])

        @pl.when(c == 0)
        def _():
            f_in[...] = jnp.zeros(f_in.shape, F32)
            f_out[...] = o_buf[...]

    step_a = (c // 2) * 4 + c % 2
    last = LAST - c
    step_s = (last // 2) * 4 + last % 2
    middle = (HUB // 2) * 4 + 4 + BLOCKS - 1

    def next_f(part):
        return f_out, f_in, "f_next", "f", d + 1, None, part

    def row_offset(part):
        return f_out, o_down, "o_hub", "o", base + HUB, None, part

    def first_offset(part):
        return f_out, eb, "down_hub", "down", base + ROW + HUB, None, part

    def first_far(part):
        return f_out, eb, "down_far", "down", base + ROW + LAST, None, part

    step_f = jnp.where(has_a, jnp.maximum(step_a + 1, 2), jnp.maximum(step_a, 1))
    step_own = jnp.where(has_a, jnp.where(c <= 1, 2, 3), 1)

    def slot(s, _):
        @pl.when(both(c > 0, has_a, s >= step_a, s < step_a + BLOCKS))
        def _():
            b = s - step_a
            some = pl.ds(pl.multiple_of(b * size, size), size)
            block_a(b).wait_recv()
            high, low = split(ina[b])
            ah[some, :] = high
            al[some, :] = low

            @pl.when(c < LAST)
            def _():
                product = dot_halves(high, low, th[...], tl[...], False)
                outa[b] = product
                block_a(b).start()

                @pl.when(c == HUB)
                def _():
                    high, low = split(product)
                    bh[some, :] = high
                    bl[some, :] = low

        @pl.when(s == step_own)
        def _():
            own_part()

        @pl.when(s == step_f)
        def _():
            for part in range(2):
                some = half(part)

                @pl.when(c > 0)
                def _():
                    received(f_in, "f", part)
                    f_out[some] = dot3(f_in[some], th[...], tl[...]) + o_buf[some]

                @pl.when(c < LAST)
                def _():
                    copy(*next_f(part)).start()

                @pl.when(both(c == LAST, r > 0, r < rows - 1))
                def _():
                    copy(*row_offset(part)).start()

                @pl.when(both(c == LAST, r == 0, r < rows - 1))
                def _():
                    copy(*first_offset(part)).start()

            @pl.when(both(c == LAST, r == 0, r < rows - 1))
            def _():
                for part in range(2):
                    copy(*first_far(part)).start()

        @pl.when(both(c < LAST, has_s, s >= step_s, s < step_s + BLOCKS))
        def _():
            b = s - step_s
            some = pl.ds(pl.multiple_of(b * size, size), size)
            block_s(b).wait_recv()
            high, low = split(ins[b])
            sh[some, :] = high
            sl[some, :] = low

            @pl.when(c > 0)
            def _():
                outs[b] = dot_halves(high, low, tth[...], ttl[...], False)
                block_s(b).start()

        @pl.when(both(s > 5, s < 8))
        def _():
            k = s - 6
            for t in range(tiles):
                lanes = slice(t * LANES, (t + 1) * LANES)
                dth[k, :, lanes] = jnp.transpose(dh[k, lanes, :])
                dtl[k, :, lanes] = jnp.transpose(dl[k, lanes, :])

        @pl.when(both(c == HUB, has_a, has_s, s > middle - tiles, s <= middle))
        def _():
            i = s - (middle - tiles + 1)
            some = pl.ds(pl.multiple_of(i * LANES, LANES), LANES)
            high, low = split(dot_halves(sh[some, :], sl[some, :], bh[...], bl[...], True))
            mh[some, :] = high
            ml[some, :] = low

        return 0

    lax.fori_loop(0, (ROW // 2 - 1) * 4 + 1 + BLOCKS, slot, 0)
    for part in range(2):
        waits.append((lambda: c < LAST, functools.partial(next_f, part)))
        waits.append(
            (lambda: both(c == LAST, r > 0, r < rows - 1), functools.partial(row_offset, part))
        )
        for late in (first_offset, first_far):
            waits.append(
                (lambda: both(c == LAST, r == 0, r < rows - 1), functools.partial(late, part))
            )

    def spread(cond, buf, name, part):
        @pl.when(c == HUB)
        def _():
            for spoke in (1, 5, HUB - 1):
                send(
                    lambda: both(cond(), c == HUB),
                    lambda spoke=spoke: (
                        buf, buf, name + str(spoke), name, base + spoke, None, part,
                    ),
                )

        @pl.when(is_spoke)
        def _():
            send(
                lambda: both(cond(), is_spoke),
                lambda: (buf, buf, name + "_pair", name, d - 1, None, part),
            )

    @pl.when(r == 0)
    def _():
        e_in[...] = f_in[...]

    @pl.when(r > 0)
    def _():
        for part in range(2):
            some = half(part)
            received(eb, "down", part)
            spread(lambda: r > 0, eb, "down", part)

            @pl.when(both(c == HUB, r < rows - 1))
            def _():
                received(o_down, "o", part)
                e_next[some] = dot3(eb[some], mh[...], ml[...], True) + o_down[some]
                send(
                    lambda: both(c == HUB, r > 0, r < rows - 1),
                    lambda part=part: (
                        e_next, eb, "down_hub", "down", base + ROW + HUB, None, part,
                    ),
                )

        @pl.when(both(c == HUB, r < rows - 1))
        def _():
            for part in range(2):
                send(
                    lambda: both(c == HUB, r > 0, r < rows - 1),
                    lambda part=part: (
                        e_next, eb, "down_far", "down", base + ROW + LAST, None, part,
                    ),
                )

        @pl.when(c == 0)
        def _():
            e_in[...] = eb[...]

        @pl.when(c > 0)
        def _():
            e_in[...] = dot3(eb[...], ah[...], al[...]) + f_in[...]

    entering = vert[0:1, :] * e_in[...]
    y[0] = dot3(g[0] + entering, dh[0], dl[0])
    y[1] = dot3(g[1] + vert[1:2, :] * y[0], dh[1], dl[1])
    halo(y, ylo, yhi, "y", 1)
    h[0] = rhs[0] - lateral_own(0, y[0]) + entering
    h[1] = rhs[1] - lateral_own(1, y[1]) + vert[1:2, :] * y[0]
    halo_received(ylo, yhi, "y")
    add_neighbours(h, ylo, yhi)

    def next_g(part):
        return g_out, g_in, "g_prev", "g", d - 1, None, part

    above = dot3(h[1], dth[1], dtl[1])
    p_buf[...] = vert[0:1, :] * dot3(h[0] + vert[1:2, :] * above, dth[0], dtl[0])

    @pl.when(c == LAST)
    def _():
        g_in[...] = jnp.zeros(g_in.shape, F32)
        g_out[...] = p_buf[...]
        for part in range(2):
            copy(*next_g(part)).start()

    @pl.when(r > 0)
    def _():
        @pl.when(c == 0)
        def _():
            w_out[...] = p_buf[...]

        @pl.when(c > 0)
        def _():
            w_out[...] = dot3(p_buf[...], ah[...], al[...], True)

        @pl.when(c == HUB - 1)
        def _():
            send(
                lambda: both(r > 0, c == HUB - 1),
                lambda: (w_out, w_pair, "w_pair", "w_pair", d + 1),
            )

        for i, other in enumerate(SPOKES + OUTER):

            @pl.when(c == other)
            def _():
                send(
                    lambda other=other: both(r > 0, c == other),
                    lambda i=i: (w_out, w_hub.at[i], "w_hub", "w" + str(i), base + HUB),
                )

        @pl.when(c == HUB)
        def _():
            received(w_pair, "w_pair")
            own = w_out[...] + w_pair[...]
            for other in range(len(SPOKES + OUTER)):
                received(w_hub.at[other], "w" + str(other))
                own = own + w_hub[other]
            o_up[...] = own

            @pl.when(r == rows - 1)
            def _():
                for name, to in (("up_hub", HUB), ("up_far", LAST)):
                    for part in range(2):
                        send(
                            lambda: both(c == HUB, r > 0, r == rows - 1),
                            lambda name=name, to=to, part=part: (
                                o_up, ub, name, "up", base - ROW + to, None, part,
                            ),
                        )

    @pl.when(c < LAST)
    def _():
        for part in range(2):
            some = half(part)
            received(g_in, "g", part)

            @pl.when(c > 0)
            def _():
                g_out[some] = dot3(g_in[some], tth[...], ttl[...]) + p_buf[some]
                copy(*next_g(part)).start()

    for part in range(2):
        waits.append((lambda: c > 0, functools.partial(next_g, part)))

    @pl.when(r < rows - 1)
    def _():
        for part in range(2):
            some = half(part)
            received(ub, "up", part)
            spread(lambda: r < rows - 1, ub, "up", part)

            @pl.when(both(c == HUB, r > 0))
            def _():
                u_next[some] = dot3(ub[some], mh[...], ml[...]) + o_up[some]
                send(
                    lambda: both(c == HUB, r > 0, r < rows - 1),
                    lambda part=part: (
                        u_next, ub, "up_hub", "up", base - ROW + HUB, None, part,
                    ),
                )

        @pl.when(both(c == HUB, r > 0))
        def _():
            for part in range(2):
                send(
                    lambda: both(c == HUB, r > 0, r < rows - 1),
                    lambda part=part: (
                        u_next, ub, "up_far", "up", base - ROW + LAST, None, part,
                    ),
                )

        @pl.when(c == LAST)
        def _():
            g_in[...] = ub[...]

        @pl.when(c < LAST)
        def _():
            g_in[...] = g_in[...] + dot3(ub[...], sh[...], sl[...])

    upper = dot3(h[1] + g_in[...], dth[1], dtl[1])
    out[1] = upper
    out[0] = dot3(h[0] + vert[1:2, :] * upper, dth[0], dtl[0])

    for cond, args in waits:
        @pl.when(cond())
        def _():
            copy(*args()).wait_send()

    @pl.when(both(c < LAST, has_a))
    def _():
        for b in range(BLOCKS):
            block_a(b).wait_send()

    @pl.when(both(c > 0, has_s))
    def _():
        for b in range(BLOCKS):
            block_s(b).wait_send()


def shards(depth, areas, rhs_field, start_field, inverses, facies, neighbours, lateral_table, vertical_table):
    layers, count, width = rhs_field.shape
    size = width // BLOCKS
    tiles = width // LANES
    field = (layers, count, width)
    matrix = (width, width)
    state = pltpu.VMEM((count, width), F32)

    def blocks():
        return pltpu.VMEM((BLOCKS, size, width), F32)

    def halves():
        return [pltpu.VMEM(matrix, BF16)] * 2

    halo = pltpu.VMEM((count, LANES), F32)
    scratch = (
        [pltpu.VMEM(field, F32)] * 2
        + [pltpu.VMEM((layers,) + matrix, F32)]
        + [pltpu.VMEM((layers,) + matrix, BF16)] * 4
        + halves() * 2
        + [blocks()] + halves() + [blocks()]
        + [blocks()] + halves() + [blocks()]
        + halves() * 2
        + [pltpu.VMEM((layers, tiles, 3 * LANES, LANES), BF16)] * 2
        + [pltpu.VMEM((neighbours.shape[1], layers, width), F32)]
        + [pltpu.VMEM((layers, width), F32)] * 2
        + [halo] * 4
        + [pltpu.VMEM((2, count, LANES), F32)] * 2
        + [state] * 2
        + [pltpu.VMEM(field, F32)] + [state] * 4
        + [state] * 3
        + [pltpu.VMEM(field, F32)] * 2
        + [state] * 3
        + [pltpu.VMEM((6, count, width), F32)] + [state]
        + [state] * 4
        + [
            pltpu.SemaphoreType.DMA((4,)),
            pltpu.SemaphoreType.DMA((len(SENDS), 2)),
            pltpu.SemaphoreType.DMA((len(RECVS), 2)),
        ]
        + [pltpu.SemaphoreType.DMA((BLOCKS,))] * 4
    )
    vmem = pl.BlockSpec(memory_space=pltpu.VMEM)
    smem = pl.BlockSpec(memory_space=pltpu.SMEM)
    hbm = pl.BlockSpec(memory_space=pl.ANY)
    return pl.pallas_call(
        functools.partial(kernel, depth, areas),
        out_shape=pltpu.VMEM(field, F32),
        in_specs=[smem, smem, vmem, vmem, hbm, hbm, hbm],
        out_specs=vmem,
        scratch_shapes=scratch,
        compiler_params=pltpu.CompilerParams(
            collective_id=0, has_side_effects=True, vmem_limit_bytes=60 * 1024 * 1024
        ),
        name="sweep",
    )(lateral_table.T, vertical_table, facies, neighbours.T, rhs_field, start_field, inverses)


def solution(mesh):
    return jax.shard_map(
        functools.partial(shards, mesh.shape["depth"], mesh.shape["area"]),
        mesh=mesh,
        in_specs=(
            P("depth", None, "area"),
            P("depth", None, "area"),
            P("depth", "area", None),
            P("depth", "area"),
            P("area", None),
            P(),
            P(),
        ),
        out_specs=P("depth", None, "area"),
        check_vma=False,
    )
```

```python
import functools

import jax
import jax.numpy as jnp
from jax import lax
from jax.experimental import pallas as pl
from jax.experimental.pallas import tpu as pltpu
from jax.sharding import PartitionSpec as P

MESH = pl.DeviceIdType.MESH
F32 = jnp.float32
BF16 = jnp.bfloat16
HW = 64
LANES = 128
ROW = 8
LAST = ROW - 1
HUB = 3
SPOKES = (7, 1, 5)
OUTER = (6, 0, 4)
BLOCKS = 8

SENDS = (
    "start_right", "start_left", "below", "f_next", "q_next", "q_far", "q_relay", "down_hub",
    "down_far", "down1", "down5", "down2", "down_pair", "y_right",
    "y_left", "w_pair", "w_hub", "g_prev", "up_hub", "up_far",
    "up1", "up5", "up2", "up_pair",
)
RECVS = (
    "start_lo", "start_hi", "below", "f", "q", "o", "down",
    "y_lo", "y_hi", "w_pair", "w0", "w1", "w2",
    "w3", "w4", "w5", "g", "up",
)


def split(x):
    high = x.astype(BF16)
    return high, (x - high.astype(F32)).astype(BF16)


def dot3(x, w_high, w_low, transposed=False):
    return dot_halves(*split(x), w_high, w_low, transposed)


def dot_halves(high, low, w_high, w_low, transposed):
    dims = (((1,), (1 if transposed else 0,)), ((), ()))
    rows = high.shape[0]
    both = lax.dot_general(
        jnp.concatenate([high, low], axis=0), w_high, dims, preferred_element_type=F32
    )
    rest = lax.dot_general(high, w_low, dims, preferred_element_type=F32)
    return both[:rows] + both[rows:] + rest


def kernel(
    depth, areas,
    lat_tab, vert_tab, facies, nbrs, rhs_hbm, start_hbm, inv_hbm,
    out,
    rhs, start, inv, dh, dl, dth, dtl, th, tl, tth, ttl, ina, ah, al, outa, ins, sh, sl, outs, bh, bl, mh, ml,
    lat_h, lat_l, wts, wsum, vert, slo, shi, ylo, yhi, to_right, to_left, below_out, below_in,
    g, f_in, f_out, o_buf, o_down, q_in, q_out, eb, e_next, e_in, y, h, p_buf, w_out, w_pair, w_hub, o_up,
    g_in, g_out, ub, u_next,
    local, snd, rcv, snd_a, rcv_a, snd_s, rcv_s,
):
    rows = depth // ROW
    d = lax.axis_index("depth")
    z = lax.axis_index("area")
    r, c = d // ROW, d % ROW
    width = out.shape[2]
    count = out.shape[1]
    tiles = width // LANES
    size = width // BLOCKS
    base = r * ROW
    has_a = r > 0
    has_s = r < rows - 1
    waits = []

    def both(*conds):
        return functools.reduce(jnp.logical_and, conds)

    def half(part):
        return pl.ds(part * (count // 2), count // 2)

    def copy(src, dst, send, recv, depth_id, area_id=None, part=None):
        if part is not None:
            src, dst = src.at[half(part)], dst.at[half(part)]
        return pltpu.make_async_remote_copy(
            src_ref=src,
            dst_ref=dst,
            send_sem=snd.at[SENDS.index(send), part or 0],
            recv_sem=rcv.at[RECVS.index(recv), part or 0],
            device_id=(depth_id, z if area_id is None else area_id),
            device_id_type=MESH,
        )

    def send(cond, args):
        waits.append((cond, args))
        copy(*args()).start()

    def received(dst, recv, part=None):
        copy(dst, dst, SENDS[0], recv, d, None, part).wait_recv()

    def block_a(b):
        return pltpu.make_async_remote_copy(
            src_ref=outa.at[b], dst_ref=ina.at[b], send_sem=snd_a.at[b], recv_sem=rcv_a.at[b],
            device_id=(d + 1, z), device_id_type=MESH,
        )

    def block_s(b):
        return pltpu.make_async_remote_copy(
            src_ref=outs.at[b], dst_ref=ins.at[b], send_sem=snd_s.at[b], recv_sem=rcv_s.at[b],
            device_id=(d - 1, z), device_id_type=MESH,
        )

    loads = [
        pltpu.make_async_copy(start_hbm, start, local.at[0]),
        pltpu.make_async_copy(inv_hbm.at[1], inv.at[1], local.at[1]),
        pltpu.make_async_copy(rhs_hbm, rhs, local.at[2]),
    ]

    def load_rows(i):
        some = pl.ds(pl.multiple_of(i * LANES, LANES), LANES)
        return pltpu.make_async_copy(inv_hbm.at[0, some], inv.at[0, some], local.at[3 + i])

    loads[0].start()
    loads[1].start()
    for i in range(tiles):
        load_rows(i).start()
    loads[2].start()

    barrier = pltpu.get_barrier_semaphore()
    is_spoke = both(c % 2 == 1, c != HUB)
    partners = [
        (d > 0, d - 1, z),
        (d < depth - 1, d + 1, z),
        (z > 0, d, z - 1),
        (z < areas - 1, d, z + 1),
        (is_spoke, base + HUB, z),
        (both(c == HUB, r > 0), d - ROW, z),
        (both(c == HUB, r < rows - 1), d + ROW, z),
        (both(c == HUB, r > 0), d - ROW + (LAST - HUB), z),
        (both(c == HUB, r < rows - 1), d + ROW + (LAST - HUB), z),
        (both(c == LAST, r > 0), d - ROW - (LAST - HUB), z),
        (both(c == LAST, r < rows - 1), d + ROW - (LAST - HUB), z),
        (both(c == LAST, r == 0, r < rows - 1), d + ROW, z),
        (both(c == LAST, r == 1), d - ROW, z),
        (c == LAST, base + 1, z),
        (c == 1, base + LAST, z),
        (both(c % 2 == 0, c != HUB - 1), base + HUB, z),
    ] + [(c == HUB, base + other, z) for other in SPOKES + OUTER]
    for cond, to_depth, to_area in partners:

        @pl.when(cond)
        def _():
            pl.semaphore_signal(
                barrier, inc=1, device_id=(to_depth, to_area), device_id_type=MESH
            )

    kinds = facies[...]
    facies_count = lat_tab.shape[1]
    v_rows = jnp.zeros(kinds.shape, F32)
    w_rows = [jnp.zeros(kinds.shape, F32) for _ in range(lat_tab.shape[0])]
    for kind in range(facies_count):
        mask = kinds == kind
        v_rows = jnp.where(mask, vert_tab[kind], v_rows)
        w_rows = [jnp.where(mask, lat_tab[j, kind], w) for j, w in enumerate(w_rows)]
    vert[...] = v_rows
    for j, w in enumerate(w_rows):
        wts[j] = w
    wsum[...] = functools.reduce(jnp.add, w_rows)

    for t in range(tiles):
        lanes = slice(t * LANES, (t + 1) * LANES)
        for k in range(2):
            for first in (0, 2 * LANES + HW):
                lat_h[k, t, first : first + HW, :] = jnp.zeros((HW, LANES), BF16)
                lat_l[k, t, first : first + HW, :] = jnp.zeros((HW, LANES), BF16)
        for first in range(HW, 2 * LANES + HW, HW):
            place = lax.broadcasted_iota(jnp.int32, (HW, LANES), 0) + (first + t * LANES - HW)
            sums = [jnp.zeros((HW, LANES), F32) for _ in range(2)]
            for j in range(nbrs.shape[0]):
                hit = place == nbrs[j : j + 1, lanes]
                for k in range(2):
                    sums[k] = sums[k] + jnp.where(hit, wts[j, k : k + 1, lanes], 0.0)
            for k in range(2):
                high, low = split(sums[k])
                lat_h[k, t, first : first + HW, :] = high
                lat_l[k, t, first : first + HW, :] = low

    def lateral_own(k, v):
        parts = [v[:, t * LANES : (t + 1) * LANES] for t in range(tiles)]
        sums = []
        for t in range(tiles):
            first, end = max(t - 1, 0), min(t + 2, tiles)
            rows_of = slice((first - t + 1) * LANES, (end - t + 1) * LANES)
            x = jnp.concatenate(parts[first:end], axis=1)
            sums.append(dot3(x, lat_h[k, t, rows_of], lat_l[k, t, rows_of]))
        return wsum[k : k + 1, :] * v - jnp.concatenate(sums, axis=1)

    def add_neighbours(field, low, high):
        for k in range(2):
            left, right = low[...], high[...]
            if k == 1:
                left, right = pltpu.roll(left, HW, 1), pltpu.roll(right, HW, 1)
            for t, x, first in ((0, left, 0), (tiles - 1, right, 2 * LANES)):
                lanes = slice(t * LANES, (t + 1) * LANES)
                rows_of = slice(first, first + LANES)
                field[k, :, lanes] = field[k, :, lanes] + dot3(
                    x, lat_h[k, t, rows_of], lat_l[k, t, rows_of]
                )

    loads[0].wait()
    below_out[...] = vert[0:1, :] * start[0]
    partner_count = sum(cond.astype(jnp.int32) for cond, _, _ in partners)
    pl.semaphore_wait(barrier, partner_count)

    has_left, has_right = z > 0, z < areas - 1

    def halo(field, low, high, name, place):
        upper_half = lax.broadcasted_iota(jnp.int32, (count, LANES), 1) >= HW

        @pl.when(has_right)
        def _():
            edge = slice(width - LANES, width)
            to_right[place] = jnp.where(
                upper_half, field[0, :, edge], pltpu.roll(field[1, :, edge], HW, 1)
            )
            send(lambda: has_right, lambda: (
                to_right.at[place], low, name + "_right", name + "_lo", d, z + 1,
            ))

        @pl.when(has_left)
        def _():
            to_left[place] = jnp.where(
                upper_half, pltpu.roll(field[1, :, :LANES], HW, 1), field[0, :, :LANES]
            )
            send(lambda: has_left, lambda: (
                to_left.at[place], high, name + "_left", name + "_hi", d, z - 1,
            ))

        @pl.when(jnp.logical_not(has_left))
        def _():
            low[...] = jnp.zeros(low.shape, F32)

        @pl.when(jnp.logical_not(has_right))
        def _():
            high[...] = jnp.zeros(high.shape, F32)

    def halo_received(low, high, name):
        @pl.when(has_left)
        def _():
            received(low, name + "_lo")

        @pl.when(has_right)
        def _():
            received(high, name + "_hi")

    halo(start, slo, shi, "start", 0)

    @pl.when(d > 0)
    def _():
        send(lambda: d > 0, lambda: (below_out, below_in, "below", "below", d - 1))

    def split_layer(k):
        def body(i, _):
            some = pl.ds(pl.multiple_of(i * LANES, LANES), LANES)
            high, low = split(inv[k, some, :])
            dh[k, some, :] = high
            dl[k, some, :] = low
            return 0

        lax.fori_loop(0, tiles, body, 0)

    per_tile = LANES // size

    def scaled_rows(some):
        scale = jnp.transpose(jnp.broadcast_to(vert[0:1, some], (LANES, LANES)))
        return inv[0, some, :] * vert[1:2, :] * jnp.concatenate([scale] * tiles, axis=1)

    def compose(i, _):
        load_rows(i).wait()
        some = pl.ds(pl.multiple_of(i * LANES, LANES), LANES)
        product = dot3(scaled_rows(some), dh[1], dl[1])
        high, low = split(product)
        th[some, :] = high
        tl[some, :] = low
        for part in range(per_tile):
            outa[i * per_tile + part] = product[part * size : (part + 1) * size]

        @pl.when(both(c == 0, has_a))
        def _():
            for part in range(per_tile):
                block_a(i * per_tile + part).start()

        return 0

    def turn(i, _):
        some = pl.ds(pl.multiple_of(i * LANES, LANES), LANES)
        tth[:, some] = jnp.transpose(th[some, :])
        ttl[:, some] = jnp.transpose(tl[some, :])
        return 0

    def halves_of_left(i, _):
        load_rows(i).wait()
        some = pl.ds(pl.multiple_of(i * LANES, LANES), LANES)
        high, low = split(scaled_rows(some))
        sh[some, :] = high
        sl[some, :] = low
        return 0

    def compose_turned(i, _):
        some = pl.ds(pl.multiple_of(i * LANES, LANES), LANES)
        product = dot3(jnp.transpose(inv[1, :, some]), sh[...], sl[...], True)
        for part in range(per_tile):
            outs[i * per_tile + part] = product[part * size : (part + 1) * size]
            block_s(i * per_tile + part).start()
        high, low = split(product)
        tth[some, :] = high
        ttl[some, :] = low
        th[:, some] = jnp.transpose(high)
        tl[:, some] = jnp.transpose(low)
        return 0

    starts_s = both(c == LAST, has_s)
    loads[1].wait()

    @pl.when(starts_s)
    def _():
        lax.fori_loop(0, tiles, halves_of_left, 0)
        lax.fori_loop(0, tiles, compose_turned, 0)
        split_layer(1)

    @pl.when(jnp.logical_not(starts_s))
    def _():
        split_layer(1)
        lax.fori_loop(0, tiles, compose, 0)

    def own_part():
        split_layer(0)
        loads[2].wait()
        g[0] = rhs[0] - lateral_own(0, start[0]) + vert[1:2, :] * start[1]
        g[1] = rhs[1] - lateral_own(1, start[1])
        halo_received(slo, shi, "start")
        add_neighbours(g, slo, shi)

        @pl.when(d < depth - 1)
        def _():
            received(below_in, "below")
            g[1] = g[1] + below_in[...]

        first = dot3(g[0], dh[0], dl[0])
        o_buf[...] = dot3(g[1] + vert[1:2, :] * first, dh[1], dl[1])

        @pl.when(c == 0)
        def _():
            f_in[...] = jnp.zeros(f_in.shape, F32)
            f_out[...] = o_buf[...]

    step_a = (c // 2) * 4 + c % 2
    last = LAST - c
    step_s = (last // 2) * 4 + last % 2

    def next_f(part):
        return f_out, f_in, "f_next", "f", d + 1, None, part

    def next_q():
        return q_out, q_in, "q_next", "q", d + 1

    def far_q():
        return q_out, q_in, "q_far", "q", base + 1

    def relay_q():
        return q_in, o_down, "q_relay", "o", base + HUB

    def first_offset(part):
        return f_out, eb, "down_hub", "down", base + ROW + HUB, None, part

    def first_far(part):
        return f_out, eb, "down_far", "down", base + ROW + LAST, None, part

    step_f = jnp.where(has_a, jnp.maximum(step_a + 1, 2), jnp.maximum(step_a, 1))
    has_q = both(has_a, has_s)
    step_q = jnp.where(c == HUB + 1, 3, jnp.where(c == HUB + 2, 4, jnp.where(c == 1, 11, c + 3)))
    step_own = jnp.where(has_a, jnp.where(c <= 1, 2, 3), 1)

    def slot(s, _):
        @pl.when(both(c > 0, has_a, s >= step_a, s < step_a + BLOCKS))
        def _():
            b = s - step_a
            some = pl.ds(pl.multiple_of(b * size, size), size)
            block_a(b).wait_recv()
            high, low = split(ina[b])
            ah[some, :] = high
            al[some, :] = low

            @pl.when(c < LAST)
            def _():
                product = dot_halves(high, low, th[...], tl[...], False)
                outa[b] = product
                block_a(b).start()

                @pl.when(c == HUB)
                def _():
                    high, low = split(product)
                    bh[some, :] = high
                    bl[some, :] = low

        @pl.when(s == step_own)
        def _():
            own_part()

        @pl.when(s == step_f)
        def _():
            for part in range(2):
                some = half(part)

                @pl.when(c > 0)
                def _():
                    received(f_in, "f", part)
                    f_out[some] = dot3(f_in[some], th[...], tl[...]) + o_buf[some]

                @pl.when(c < LAST)
                def _():
                    copy(*next_f(part)).start()

                @pl.when(both(c == LAST, r == 0, r < rows - 1))
                def _():
                    copy(*first_offset(part)).start()

            @pl.when(both(c == LAST, r == 0, r < rows - 1))
            def _():
                for part in range(2):
                    copy(*first_far(part)).start()

        @pl.when(both(has_q, s == step_q))
        def _():
            @pl.when(c == HUB + 1)
            def _():
                q_out[...] = o_buf[...]

            @pl.when(c > HUB + 1)
            def _():
                received(q_in, "q")
                q_out[...] = dot3(q_in[...], th[...], tl[...]) + o_buf[...]

            @pl.when(both(c > HUB, c < LAST))
            def _():
                copy(*next_q()).start()

            @pl.when(c == LAST)
            def _():
                copy(*far_q()).start()

            @pl.when(c == 1)
            def _():
                received(q_in, "q")
                copy(*relay_q()).start()

        @pl.when(both(s == 4, jnp.logical_not(starts_s)))
        def _():
            lax.fori_loop(0, tiles, turn, 0)

        @pl.when(both(c < LAST, has_s, s >= step_s, s < step_s + BLOCKS))
        def _():
            b = s - step_s
            some = pl.ds(pl.multiple_of(b * size, size), size)
            block_s(b).wait_recv()
            high, low = split(ins[b])
            sh[some, :] = high
            sl[some, :] = low

            @pl.when(c == LAST - 1)
            def _():
                outs[b] = dot_halves(high, low, th[...], tl[...], True)
                block_s(b).start()

            @pl.when(both(c > 0, c < LAST - 1))
            def _():
                outs[b] = dot_halves(high, low, tth[...], ttl[...], False)
                block_s(b).start()

        @pl.when(both(s > 5, s < 8))
        def _():
            k = s - 6
            for t in range(tiles):
                lanes = slice(t * LANES, (t + 1) * LANES)
                dth[k, :, lanes] = jnp.transpose(dh[k, lanes, :])
                dtl[k, :, lanes] = jnp.transpose(dl[k, lanes, :])

        return 0

    lax.fori_loop(0, (ROW // 2 - 1) * 4 + 1 + BLOCKS, slot, 0)
    waits.append((lambda: both(has_q, c > HUB, c < LAST), next_q))
    waits.append((lambda: both(has_q, c == LAST), far_q))
    waits.append((lambda: both(has_q, c == 1), relay_q))
    for part in range(2):
        waits.append((lambda: c < LAST, functools.partial(next_f, part)))
        for late in (first_offset, first_far):
            waits.append(
                (lambda: both(c == LAST, r == 0, r < rows - 1), functools.partial(late, part))
            )

    def spread(cond, buf, name, part):
        @pl.when(c == HUB)
        def _():
            for spoke in (1, 5, HUB - 1):
                send(
                    lambda: both(cond(), c == HUB),
                    lambda spoke=spoke: (
                        buf, buf, name + str(spoke), name, base + spoke, None, part,
                    ),
                )

        @pl.when(is_spoke)
        def _():
            send(
                lambda: both(cond(), is_spoke),
                lambda: (buf, buf, name + "_pair", name, d - 1, None, part),
            )

    @pl.when(r == 0)
    def _():
        e_in[...] = f_in[...]

    @pl.when(r > 0)
    def _():
        @pl.when(both(c == HUB, r < rows - 1))
        def _():
            received(o_down, "o")

        for part in range(2):
            some = half(part)
            received(eb, "down", part)
            spread(lambda: r > 0, eb, "down", part)

            @pl.when(both(c == HUB, r < rows - 1))
            def _():
                across = dot3(eb[some], bh[...], bl[...]) + f_out[some]
                e_next[some] = dot3(across, sh[...], sl[...], True) + o_down[some]
                send(
                    lambda: both(c == HUB, r > 0, r < rows - 1),
                    lambda part=part: (
                        e_next, eb, "down_hub", "down", base + ROW + HUB, None, part,
                    ),
                )

        @pl.when(both(c == HUB, r < rows - 1))
        def _():
            for part in range(2):
                send(
                    lambda: both(c == HUB, r > 0, r < rows - 1),
                    lambda part=part: (
                        e_next, eb, "down_far", "down", base + ROW + LAST, None, part,
                    ),
                )

            def product(i, _):
                some = pl.ds(pl.multiple_of(i * LANES, LANES), LANES)
                high, low = split(dot_halves(sh[some, :], sl[some, :], bh[...], bl[...], True))
                mh[some, :] = high
                ml[some, :] = low
                return 0

            lax.fori_loop(0, tiles, product, 0)

        @pl.when(c == 0)
        def _():
            e_in[...] = eb[...]

        @pl.when(c > 0)
        def _():
            e_in[...] = dot3(eb[...], ah[...], al[...]) + f_in[...]

    entering = vert[0:1, :] * e_in[...]
    y[0] = dot3(g[0] + entering, dh[0], dl[0])
    y[1] = dot3(g[1] + vert[1:2, :] * y[0], dh[1], dl[1])
    halo(y, ylo, yhi, "y", 1)
    h[0] = rhs[0] - lateral_own(0, y[0]) + entering
    h[1] = rhs[1] - lateral_own(1, y[1]) + vert[1:2, :] * y[0]
    halo_received(ylo, yhi, "y")
    add_neighbours(h, ylo, yhi)

    def next_g(part):
        return g_out, g_in, "g_prev", "g", d - 1, None, part

    above = dot3(h[1], dth[1], dtl[1])
    p_buf[...] = vert[0:1, :] * dot3(h[0] + vert[1:2, :] * above, dth[0], dtl[0])

    @pl.when(c == LAST)
    def _():
        g_in[...] = jnp.zeros(g_in.shape, F32)
        g_out[...] = p_buf[...]
        for part in range(2):
            copy(*next_g(part)).start()

    @pl.when(r > 0)
    def _():
        @pl.when(c == 0)
        def _():
            w_out[...] = p_buf[...]

        @pl.when(c > 0)
        def _():
            w_out[...] = dot3(p_buf[...], ah[...], al[...], True)

        @pl.when(c == HUB - 1)
        def _():
            send(
                lambda: both(r > 0, c == HUB - 1),
                lambda: (w_out, w_pair, "w_pair", "w_pair", d + 1),
            )

        for i, other in enumerate(SPOKES + OUTER):

            @pl.when(c == other)
            def _():
                send(
                    lambda other=other: both(r > 0, c == other),
                    lambda i=i: (w_out, w_hub.at[i], "w_hub", "w" + str(i), base + HUB),
                )

        @pl.when(c == HUB)
        def _():
            received(w_pair, "w_pair")
            own = w_out[...] + w_pair[...]
            for other in range(len(SPOKES + OUTER)):
                received(w_hub.at[other], "w" + str(other))
                own = own + w_hub[other]
            o_up[...] = own

            @pl.when(r == rows - 1)
            def _():
                for name, to in (("up_hub", HUB), ("up_far", LAST)):
                    for part in range(2):
                        send(
                            lambda: both(c == HUB, r > 0, r == rows - 1),
                            lambda name=name, to=to, part=part: (
                                o_up, ub, name, "up", base - ROW + to, None, part,
                            ),
                        )

    @pl.when(c < LAST)
    def _():
        for part in range(2):
            some = half(part)
            received(g_in, "g", part)

            @pl.when(c > 0)
            def _():
                g_out[some] = dot3(g_in[some], tth[...], ttl[...]) + p_buf[some]
                copy(*next_g(part)).start()

    for part in range(2):
        waits.append((lambda: c > 0, functools.partial(next_g, part)))

    @pl.when(r < rows - 1)
    def _():
        for part in range(2):
            some = half(part)
            received(ub, "up", part)
            spread(lambda: r < rows - 1, ub, "up", part)

            @pl.when(both(c == HUB, r > 0))
            def _():
                u_next[some] = dot3(ub[some], mh[...], ml[...]) + o_up[some]
                send(
                    lambda: both(c == HUB, r > 0, r < rows - 1),
                    lambda part=part: (
                        u_next, ub, "up_hub", "up", base - ROW + HUB, None, part,
                    ),
                )

        @pl.when(both(c == HUB, r > 0))
        def _():
            for part in range(2):
                send(
                    lambda: both(c == HUB, r > 0, r < rows - 1),
                    lambda part=part: (
                        u_next, ub, "up_far", "up", base - ROW + LAST, None, part,
                    ),
                )

        @pl.when(c == LAST)
        def _():
            g_in[...] = ub[...]

        @pl.when(c < LAST)
        def _():
            g_in[...] = g_in[...] + dot3(ub[...], sh[...], sl[...])

    upper = dot3(h[1] + g_in[...], dth[1], dtl[1])
    out[1] = upper
    out[0] = dot3(h[0] + vert[1:2, :] * upper, dth[0], dtl[0])

    for cond, args in waits:
        @pl.when(cond())
        def _():
            copy(*args()).wait_send()

    @pl.when(both(c < LAST, has_a))
    def _():
        for b in range(BLOCKS):
            block_a(b).wait_send()

    @pl.when(both(c > 0, has_s))
    def _():
        for b in range(BLOCKS):
            block_s(b).wait_send()


def shards(depth, areas, rhs_field, start_field, inverses, facies, neighbours, lateral_table, vertical_table):
    layers, count, width = rhs_field.shape
    size = width // BLOCKS
    tiles = width // LANES
    field = (layers, count, width)
    matrix = (width, width)
    state = pltpu.VMEM((count, width), F32)

    def blocks():
        return pltpu.VMEM((BLOCKS, size, width), F32)

    def halves():
        return [pltpu.VMEM(matrix, BF16)] * 2

    halo = pltpu.VMEM((count, LANES), F32)
    scratch = (
        [pltpu.VMEM(field, F32)] * 2
        + [pltpu.VMEM((layers,) + matrix, F32)]
        + [pltpu.VMEM((layers,) + matrix, BF16)] * 4
        + halves() * 2
        + [blocks()] + halves() + [blocks()]
        + [blocks()] + halves() + [blocks()]
        + halves() * 2
        + [pltpu.VMEM((layers, tiles, 3 * LANES, LANES), BF16)] * 2
        + [pltpu.VMEM((neighbours.shape[1], layers, width), F32)]
        + [pltpu.VMEM((layers, width), F32)] * 2
        + [halo] * 4
        + [pltpu.VMEM((2, count, LANES), F32)] * 2
        + [state] * 2
        + [pltpu.VMEM(field, F32)] + [state] * 6
        + [state] * 3
        + [pltpu.VMEM(field, F32)] * 2
        + [state] * 3
        + [pltpu.VMEM((6, count, width), F32)] + [state]
        + [state] * 4
        + [
            pltpu.SemaphoreType.DMA((3 + tiles,)),
            pltpu.SemaphoreType.DMA((len(SENDS), 2)),
            pltpu.SemaphoreType.DMA((len(RECVS), 2)),
        ]
        + [pltpu.SemaphoreType.DMA((BLOCKS,))] * 4
    )
    vmem = pl.BlockSpec(memory_space=pltpu.VMEM)
    smem = pl.BlockSpec(memory_space=pltpu.SMEM)
    hbm = pl.BlockSpec(memory_space=pl.ANY)
    return pl.pallas_call(
        functools.partial(kernel, depth, areas),
        out_shape=pltpu.VMEM(field, F32),
        in_specs=[smem, smem, vmem, vmem, hbm, hbm, hbm],
        out_specs=vmem,
        scratch_shapes=scratch,
        compiler_params=pltpu.CompilerParams(
            collective_id=0, has_side_effects=True, vmem_limit_bytes=60 * 1024 * 1024
        ),
        name="sweep",
    )(lateral_table.T, vertical_table, facies, neighbours.T, rhs_field, start_field, inverses)


def solution(mesh):
    return jax.shard_map(
        functools.partial(shards, mesh.shape["depth"], mesh.shape["area"]),
        mesh=mesh,
        in_specs=(
            P("depth", None, "area"),
            P("depth", None, "area"),
            P("depth", "area", None),
            P("depth", "area"),
            P("area", None),
            P(),
            P(),
        ),
        out_specs=P("depth", None, "area"),
        check_vma=False,
    )
```

```python
import functools

import jax
import jax.numpy as jnp
from jax import lax
from jax.experimental import pallas as pl
from jax.experimental.pallas import tpu as pltpu
from jax.sharding import PartitionSpec as P

MESH = pl.DeviceIdType.MESH
F32 = jnp.float32
BF16 = jnp.bfloat16
HW = 64
LANES = 128
ROW = 8
LAST = ROW - 1
HUB = 3
SPOKES = (7, 1, 5)
OUTER = (6, 0, 4)
BLOCKS = 8

SENDS = (
    "start_right", "start_left", "below", "f_next", "q_next", "q_far", "q_relay", "down_hub",
    "down_far", "down1", "down5", "down2", "down_pair", "y_right",
    "y_left", "w_pair", "w_hub", "g_prev", "up_hub", "up_far",
    "up1", "up5", "up2", "up_pair",
)
RECVS = (
    "start_lo", "start_hi", "below", "f", "q", "o", "down",
    "y_lo", "y_hi", "w_pair", "w0", "w1", "w2",
    "w3", "w4", "w5", "g", "up",
)


def split(x):
    high = x.astype(BF16)
    return high, (x - high.astype(F32)).astype(BF16)


def dot3(x, w_high, w_low, transposed=False):
    return dot_halves(*split(x), w_high, w_low, transposed)


def dot_halves(high, low, w_high, w_low, transposed):
    dims = (((1,), (1 if transposed else 0,)), ((), ()))
    rows = high.shape[0]
    both = lax.dot_general(
        jnp.concatenate([high, low], axis=0), w_high, dims, preferred_element_type=F32
    )
    rest = lax.dot_general(high, w_low, dims, preferred_element_type=F32)
    return both[:rows] + both[rows:] + rest


def kernel(
    depth, areas,
    lat_tab_hbm, vert_tab_hbm, facies_hbm, nbrs_hbm, rhs_hbm, start_hbm, inv_hbm,
    out,
    lat_tab, vert_tab, facies, nbrs, rhs, start, inv, dh, dl, dth, dtl, th, tl, tth, ttl, ina, ah, al, outa, ins, sh, sl, outs, bh, bl, mh, ml,
    lat_h, lat_l, wts, wsum, vert, slo, shi, ylo, yhi, to_right, to_left, below_out, below_in,
    g, f_in, f_out, o_buf, o_down, q_in, q_out, eb, e_next, e_in, y, h, p_buf, w_out, w_pair, w_hub, o_up,
    g_in, g_out, ub, u_next,
    local, snd, rcv, snd_a, rcv_a, snd_s, rcv_s,
):
    rows = depth // ROW
    d = lax.axis_index("depth")
    z = lax.axis_index("area")
    r, c = d // ROW, d % ROW
    width = out.shape[2]
    count = out.shape[1]
    tiles = width // LANES
    size = width // BLOCKS
    base = r * ROW
    has_a = r > 0
    has_s = r < rows - 1
    waits = []

    def both(*conds):
        return functools.reduce(jnp.logical_and, conds)

    def half(part):
        return pl.ds(part * (count // 2), count // 2)

    def copy(src, dst, send, recv, depth_id, area_id=None, part=None):
        if part is not None:
            src, dst = src.at[half(part)], dst.at[half(part)]
        return pltpu.make_async_remote_copy(
            src_ref=src,
            dst_ref=dst,
            send_sem=snd.at[SENDS.index(send), part or 0],
            recv_sem=rcv.at[RECVS.index(recv), part or 0],
            device_id=(depth_id, z if area_id is None else area_id),
            device_id_type=MESH,
        )

    def send(cond, args):
        waits.append((cond, args))
        copy(*args()).start()

    def received(dst, recv, part=None):
        copy(dst, dst, SENDS[0], recv, d, None, part).wait_recv()

    def block_a(b):
        return pltpu.make_async_remote_copy(
            src_ref=outa.at[b], dst_ref=ina.at[b], send_sem=snd_a.at[b], recv_sem=rcv_a.at[b],
            device_id=(d + 1, z), device_id_type=MESH,
        )

    def block_s(b):
        return pltpu.make_async_remote_copy(
            src_ref=outs.at[b], dst_ref=ins.at[b], send_sem=snd_s.at[b], recv_sem=rcv_s.at[b],
            device_id=(d - 1, z), device_id_type=MESH,
        )

    loads = [
        pltpu.make_async_copy(start_hbm, start, local.at[0]),
        pltpu.make_async_copy(inv_hbm.at[1], inv.at[1], local.at[1]),
        pltpu.make_async_copy(rhs_hbm, rhs, local.at[2]),
    ]

    def load_rows(i):
        some = pl.ds(pl.multiple_of(i * LANES, LANES), LANES)
        return pltpu.make_async_copy(inv_hbm.at[0, some], inv.at[0, some], local.at[3 + i])

    small = [
        pltpu.make_async_copy(source, target, local.at[3 + tiles + i])
        for i, (source, target) in enumerate(
            ((facies_hbm, facies), (nbrs_hbm, nbrs), (lat_tab_hbm, lat_tab), (vert_tab_hbm, vert_tab))
        )
    ]
    for load in small:
        load.start()
    loads[0].start()
    loads[1].start()
    for i in range(tiles):
        load_rows(i).start()
    loads[2].start()

    barrier = pltpu.get_barrier_semaphore()
    is_spoke = both(c % 2 == 1, c != HUB)
    partners = [
        (d > 0, d - 1, z),
        (d < depth - 1, d + 1, z),
        (z > 0, d, z - 1),
        (z < areas - 1, d, z + 1),
        (is_spoke, base + HUB, z),
        (both(c == HUB, r > 0), d - ROW, z),
        (both(c == HUB, r < rows - 1), d + ROW, z),
        (both(c == HUB, r > 0), d - ROW + (LAST - HUB), z),
        (both(c == HUB, r < rows - 1), d + ROW + (LAST - HUB), z),
        (both(c == LAST, r > 0), d - ROW - (LAST - HUB), z),
        (both(c == LAST, r < rows - 1), d + ROW - (LAST - HUB), z),
        (both(c == LAST, r == 0, r < rows - 1), d + ROW, z),
        (both(c == LAST, r == 1), d - ROW, z),
        (c == LAST, base + 1, z),
        (c == 1, base + LAST, z),
        (both(c % 2 == 0, c != HUB - 1), base + HUB, z),
    ] + [(c == HUB, base + other, z) for other in SPOKES + OUTER]
    for cond, to_depth, to_area in partners:

        @pl.when(cond)
        def _():
            pl.semaphore_signal(
                barrier, inc=1, device_id=(to_depth, to_area), device_id_type=MESH
            )

    for load in small:
        load.wait()
    kinds = facies[...]
    facies_count = lat_tab.shape[1]
    v_rows = jnp.zeros(kinds.shape, F32)
    w_rows = [jnp.zeros(kinds.shape, F32) for _ in range(lat_tab.shape[0])]
    for kind in range(facies_count):
        mask = kinds == kind
        v_rows = jnp.where(mask, vert_tab[kind], v_rows)
        w_rows = [jnp.where(mask, lat_tab[j, kind], w) for j, w in enumerate(w_rows)]
    vert[...] = v_rows
    for j, w in enumerate(w_rows):
        wts[j] = w
    wsum[...] = functools.reduce(jnp.add, w_rows)

    for t in range(tiles):
        lanes = slice(t * LANES, (t + 1) * LANES)
        for k in range(2):
            for first in (0, 2 * LANES + HW):
                lat_h[k, t, first : first + HW, :] = jnp.zeros((HW, LANES), BF16)
                lat_l[k, t, first : first + HW, :] = jnp.zeros((HW, LANES), BF16)
        for first in range(HW, 2 * LANES + HW, HW):
            place = lax.broadcasted_iota(jnp.int32, (HW, LANES), 0) + (first + t * LANES - HW)
            sums = [jnp.zeros((HW, LANES), F32) for _ in range(2)]
            for j in range(nbrs.shape[0]):
                hit = place == nbrs[j : j + 1, lanes]
                for k in range(2):
                    sums[k] = sums[k] + jnp.where(hit, wts[j, k : k + 1, lanes], 0.0)
            for k in range(2):
                high, low = split(sums[k])
                lat_h[k, t, first : first + HW, :] = high
                lat_l[k, t, first : first + HW, :] = low

    def lateral_own(k, v):
        parts = [v[:, t * LANES : (t + 1) * LANES] for t in range(tiles)]
        sums = []
        for t in range(tiles):
            first, end = max(t - 1, 0), min(t + 2, tiles)
            rows_of = slice((first - t + 1) * LANES, (end - t + 1) * LANES)
            x = jnp.concatenate(parts[first:end], axis=1)
            sums.append(dot3(x, lat_h[k, t, rows_of], lat_l[k, t, rows_of]))
        return wsum[k : k + 1, :] * v - jnp.concatenate(sums, axis=1)

    def add_neighbours(field, low, high):
        for k in range(2):
            left, right = low[...], high[...]
            if k == 1:
                left, right = pltpu.roll(left, HW, 1), pltpu.roll(right, HW, 1)
            for t, x, first in ((0, left, 0), (tiles - 1, right, 2 * LANES)):
                lanes = slice(t * LANES, (t + 1) * LANES)
                rows_of = slice(first, first + LANES)
                field[k, :, lanes] = field[k, :, lanes] + dot3(
                    x, lat_h[k, t, rows_of], lat_l[k, t, rows_of]
                )

    loads[0].wait()
    below_out[...] = vert[0:1, :] * start[0]
    partner_count = sum(cond.astype(jnp.int32) for cond, _, _ in partners)
    pl.semaphore_wait(barrier, partner_count)

    has_left, has_right = z > 0, z < areas - 1

    def halo(field, low, high, name, place):
        upper_half = lax.broadcasted_iota(jnp.int32, (count, LANES), 1) >= HW

        @pl.when(has_right)
        def _():
            edge = slice(width - LANES, width)
            to_right[place] = jnp.where(
                upper_half, field[0, :, edge], pltpu.roll(field[1, :, edge], HW, 1)
            )
            send(lambda: has_right, lambda: (
                to_right.at[place], low, name + "_right", name + "_lo", d, z + 1,
            ))

        @pl.when(has_left)
        def _():
            to_left[place] = jnp.where(
                upper_half, pltpu.roll(field[1, :, :LANES], HW, 1), field[0, :, :LANES]
            )
            send(lambda: has_left, lambda: (
                to_left.at[place], high, name + "_left", name + "_hi", d, z - 1,
            ))

        @pl.when(jnp.logical_not(has_left))
        def _():
            low[...] = jnp.zeros(low.shape, F32)

        @pl.when(jnp.logical_not(has_right))
        def _():
            high[...] = jnp.zeros(high.shape, F32)

    def halo_received(low, high, name):
        @pl.when(has_left)
        def _():
            received(low, name + "_lo")

        @pl.when(has_right)
        def _():
            received(high, name + "_hi")

    halo(start, slo, shi, "start", 0)

    @pl.when(d > 0)
    def _():
        send(lambda: d > 0, lambda: (below_out, below_in, "below", "below", d - 1))

    def split_layer(k):
        def body(i, _):
            some = pl.ds(pl.multiple_of(i * LANES, LANES), LANES)
            high, low = split(inv[k, some, :])
            dh[k, some, :] = high
            dl[k, some, :] = low
            return 0

        lax.fori_loop(0, tiles, body, 0)

    per_tile = LANES // size

    def scaled_rows(some):
        scale = jnp.transpose(jnp.broadcast_to(vert[0:1, some], (LANES, LANES)))
        return inv[0, some, :] * vert[1:2, :] * jnp.concatenate([scale] * tiles, axis=1)

    def compose(i, _):
        load_rows(i).wait()
        some = pl.ds(pl.multiple_of(i * LANES, LANES), LANES)
        product = dot3(scaled_rows(some), dh[1], dl[1])
        high, low = split(product)
        th[some, :] = high
        tl[some, :] = low
        for part in range(per_tile):
            outa[i * per_tile + part] = product[part * size : (part + 1) * size]

        @pl.when(both(c == 0, has_a))
        def _():
            for part in range(per_tile):
                block_a(i * per_tile + part).start()

        return 0

    def turn(i, _):
        some = pl.ds(pl.multiple_of(i * LANES, LANES), LANES)
        tth[:, some] = jnp.transpose(th[some, :])
        ttl[:, some] = jnp.transpose(tl[some, :])
        return 0

    def halves_of_left(i, _):
        load_rows(i).wait()
        some = pl.ds(pl.multiple_of(i * LANES, LANES), LANES)
        high, low = split(scaled_rows(some))
        sh[some, :] = high
        sl[some, :] = low
        return 0

    def compose_turned(i, _):
        some = pl.ds(pl.multiple_of(i * LANES, LANES), LANES)
        product = dot3(jnp.transpose(inv[1, :, some]), sh[...], sl[...], True)
        for part in range(per_tile):
            outs[i * per_tile + part] = product[part * size : (part + 1) * size]
            block_s(i * per_tile + part).start()
        high, low = split(product)
        tth[some, :] = high
        ttl[some, :] = low
        th[:, some] = jnp.transpose(high)
        tl[:, some] = jnp.transpose(low)
        return 0

    starts_s = both(c == LAST, has_s)
    loads[1].wait()

    @pl.when(starts_s)
    def _():
        lax.fori_loop(0, tiles, halves_of_left, 0)
        lax.fori_loop(0, tiles, compose_turned, 0)
        split_layer(1)

    @pl.when(jnp.logical_not(starts_s))
    def _():
        split_layer(1)
        lax.fori_loop(0, tiles, compose, 0)

    def own_part():
        split_layer(0)
        loads[2].wait()
        g[0] = rhs[0] - lateral_own(0, start[0]) + vert[1:2, :] * start[1]
        g[1] = rhs[1] - lateral_own(1, start[1])
        halo_received(slo, shi, "start")
        add_neighbours(g, slo, shi)

        @pl.when(d < depth - 1)
        def _():
            received(below_in, "below")
            g[1] = g[1] + below_in[...]

        first = dot3(g[0], dh[0], dl[0])
        o_buf[...] = dot3(g[1] + vert[1:2, :] * first, dh[1], dl[1])

        @pl.when(c == 0)
        def _():
            f_in[...] = jnp.zeros(f_in.shape, F32)
            f_out[...] = o_buf[...]

    step_a = (c // 2) * 4 + c % 2
    last = LAST - c
    step_s = (last // 2) * 4 + last % 2

    def next_f(part):
        return f_out, f_in, "f_next", "f", d + 1, None, part

    def next_q():
        return q_out, q_in, "q_next", "q", d + 1

    def far_q():
        return q_out, q_in, "q_far", "q", base + 1

    def relay_q():
        return q_in, o_down, "q_relay", "o", base + HUB

    def first_offset(part):
        return f_out, eb, "down_hub", "down", base + ROW + HUB, None, part

    def first_far(part):
        return f_out, eb, "down_far", "down", base + ROW + LAST, None, part

    step_f = jnp.where(has_a, jnp.maximum(step_a + 1, 2), jnp.maximum(step_a, 1))
    has_q = both(has_a, has_s)
    step_q = jnp.where(c == HUB + 1, 3, jnp.where(c == HUB + 2, 4, jnp.where(c == 1, 11, c + 3)))
    step_own = jnp.where(has_a, jnp.where(c <= 1, 2, 3), 1)

    def slot(s, _):
        @pl.when(both(c > 0, has_a, s >= step_a, s < step_a + BLOCKS))
        def _():
            b = s - step_a
            some = pl.ds(pl.multiple_of(b * size, size), size)
            block_a(b).wait_recv()
            high, low = split(ina[b])
            ah[some, :] = high
            al[some, :] = low

            @pl.when(c < LAST)
            def _():
                product = dot_halves(high, low, th[...], tl[...], False)
                outa[b] = product
                block_a(b).start()

                @pl.when(c == HUB)
                def _():
                    high, low = split(product)
                    bh[some, :] = high
                    bl[some, :] = low

        @pl.when(s == step_own)
        def _():
            own_part()

        @pl.when(s == step_f)
        def _():
            for part in range(2):
                some = half(part)

                @pl.when(c > 0)
                def _():
                    received(f_in, "f", part)
                    f_out[some] = dot3(f_in[some], th[...], tl[...]) + o_buf[some]

                @pl.when(c < LAST)
                def _():
                    copy(*next_f(part)).start()

                @pl.when(both(c == LAST, r == 0, r < rows - 1))
                def _():
                    copy(*first_offset(part)).start()

            @pl.when(both(c == LAST, r == 0, r < rows - 1))
            def _():
                for part in range(2):
                    copy(*first_far(part)).start()

        @pl.when(both(has_q, s == step_q))
        def _():
            @pl.when(c == HUB + 1)
            def _():
                q_out[...] = o_buf[...]

            @pl.when(c > HUB + 1)
            def _():
                received(q_in, "q")
                q_out[...] = dot3(q_in[...], th[...], tl[...]) + o_buf[...]

            @pl.when(both(c > HUB, c < LAST))
            def _():
                copy(*next_q()).start()

            @pl.when(c == LAST)
            def _():
                copy(*far_q()).start()

            @pl.when(c == 1)
            def _():
                received(q_in, "q")
                copy(*relay_q()).start()

        @pl.when(both(s == 4, jnp.logical_not(starts_s)))
        def _():
            lax.fori_loop(0, tiles, turn, 0)

        @pl.when(both(c < LAST, has_s, s >= step_s, s < step_s + BLOCKS))
        def _():
            b = s - step_s
            some = pl.ds(pl.multiple_of(b * size, size), size)
            block_s(b).wait_recv()
            high, low = split(ins[b])
            sh[some, :] = high
            sl[some, :] = low

            @pl.when(c == LAST - 1)
            def _():
                outs[b] = dot_halves(high, low, th[...], tl[...], True)
                block_s(b).start()

            @pl.when(both(c > 0, c < LAST - 1))
            def _():
                outs[b] = dot_halves(high, low, tth[...], ttl[...], False)
                block_s(b).start()

        @pl.when(both(s > 5, s < 8))
        def _():
            k = s - 6
            for t in range(tiles):
                lanes = slice(t * LANES, (t + 1) * LANES)
                dth[k, :, lanes] = jnp.transpose(dh[k, lanes, :])
                dtl[k, :, lanes] = jnp.transpose(dl[k, lanes, :])

        return 0

    lax.fori_loop(0, (ROW // 2 - 1) * 4 + 1 + BLOCKS, slot, 0)
    waits.append((lambda: both(has_q, c > HUB, c < LAST), next_q))
    waits.append((lambda: both(has_q, c == LAST), far_q))
    waits.append((lambda: both(has_q, c == 1), relay_q))
    for part in range(2):
        waits.append((lambda: c < LAST, functools.partial(next_f, part)))
        for late in (first_offset, first_far):
            waits.append(
                (lambda: both(c == LAST, r == 0, r < rows - 1), functools.partial(late, part))
            )

    def spread(cond, buf, name, part):
        @pl.when(c == HUB)
        def _():
            for spoke in (1, 5, HUB - 1):
                send(
                    lambda: both(cond(), c == HUB),
                    lambda spoke=spoke: (
                        buf, buf, name + str(spoke), name, base + spoke, None, part,
                    ),
                )

        @pl.when(is_spoke)
        def _():
            send(
                lambda: both(cond(), is_spoke),
                lambda: (buf, buf, name + "_pair", name, d - 1, None, part),
            )

    @pl.when(r == 0)
    def _():
        e_in[...] = f_in[...]

    @pl.when(r > 0)
    def _():
        @pl.when(both(c == HUB, r < rows - 1))
        def _():
            received(o_down, "o")

        for part in range(2):
            some = half(part)
            received(eb, "down", part)
            spread(lambda: r > 0, eb, "down", part)

            @pl.when(both(c == HUB, r < rows - 1))
            def _():
                across = dot3(eb[some], bh[...], bl[...]) + f_out[some]
                e_next[some] = dot3(across, sh[...], sl[...], True) + o_down[some]
                send(
                    lambda: both(c == HUB, r > 0, r < rows - 1),
                    lambda part=part: (
                        e_next, eb, "down_hub", "down", base + ROW + HUB, None, part,
                    ),
                )

        @pl.when(both(c == HUB, r < rows - 1))
        def _():
            for part in range(2):
                send(
                    lambda: both(c == HUB, r > 0, r < rows - 1),
                    lambda part=part: (
                        e_next, eb, "down_far", "down", base + ROW + LAST, None, part,
                    ),
                )

            def product(i, _):
                some = pl.ds(pl.multiple_of(i * LANES, LANES), LANES)
                high, low = split(dot_halves(sh[some, :], sl[some, :], bh[...], bl[...], True))
                mh[some, :] = high
                ml[some, :] = low
                return 0

            lax.fori_loop(0, tiles, product, 0)

        @pl.when(c == 0)
        def _():
            e_in[...] = eb[...]

        @pl.when(c > 0)
        def _():
            e_in[...] = dot3(eb[...], ah[...], al[...]) + f_in[...]

    entering = vert[0:1, :] * e_in[...]
    y[0] = dot3(g[0] + entering, dh[0], dl[0])
    y[1] = dot3(g[1] + vert[1:2, :] * y[0], dh[1], dl[1])
    halo(y, ylo, yhi, "y", 1)
    h[0] = rhs[0] - lateral_own(0, y[0]) + entering
    h[1] = rhs[1] - lateral_own(1, y[1]) + vert[1:2, :] * y[0]
    halo_received(ylo, yhi, "y")
    add_neighbours(h, ylo, yhi)

    def next_g(part):
        return g_out, g_in, "g_prev", "g", d - 1, None, part

    above = dot3(h[1], dth[1], dtl[1])
    p_buf[...] = vert[0:1, :] * dot3(h[0] + vert[1:2, :] * above, dth[0], dtl[0])

    @pl.when(c == LAST)
    def _():
        g_in[...] = jnp.zeros(g_in.shape, F32)
        g_out[...] = p_buf[...]
        for part in range(2):
            copy(*next_g(part)).start()

    @pl.when(r > 0)
    def _():
        @pl.when(c == 0)
        def _():
            w_out[...] = p_buf[...]

        @pl.when(c > 0)
        def _():
            w_out[...] = dot3(p_buf[...], ah[...], al[...], True)

        @pl.when(c == HUB - 1)
        def _():
            send(
                lambda: both(r > 0, c == HUB - 1),
                lambda: (w_out, w_pair, "w_pair", "w_pair", d + 1),
            )

        for i, other in enumerate(SPOKES + OUTER):

            @pl.when(c == other)
            def _():
                send(
                    lambda other=other: both(r > 0, c == other),
                    lambda i=i: (w_out, w_hub.at[i], "w_hub", "w" + str(i), base + HUB),
                )

        @pl.when(c == HUB)
        def _():
            received(w_pair, "w_pair")
            own = w_out[...] + w_pair[...]
            for other in range(len(SPOKES + OUTER)):
                received(w_hub.at[other], "w" + str(other))
                own = own + w_hub[other]
            o_up[...] = own

            @pl.when(r == rows - 1)
            def _():
                for name, to in (("up_hub", HUB), ("up_far", LAST)):
                    for part in range(2):
                        send(
                            lambda: both(c == HUB, r > 0, r == rows - 1),
                            lambda name=name, to=to, part=part: (
                                o_up, ub, name, "up", base - ROW + to, None, part,
                            ),
                        )

    @pl.when(c < LAST)
    def _():
        for part in range(2):
            some = half(part)
            received(g_in, "g", part)

            @pl.when(c > 0)
            def _():
                g_out[some] = dot3(g_in[some], tth[...], ttl[...]) + p_buf[some]
                copy(*next_g(part)).start()

    for part in range(2):
        waits.append((lambda: c > 0, functools.partial(next_g, part)))

    @pl.when(r < rows - 1)
    def _():
        for part in range(2):
            some = half(part)
            received(ub, "up", part)
            spread(lambda: r < rows - 1, ub, "up", part)

            @pl.when(both(c == HUB, r > 0))
            def _():
                u_next[some] = dot3(ub[some], mh[...], ml[...]) + o_up[some]
                send(
                    lambda: both(c == HUB, r > 0, r < rows - 1),
                    lambda part=part: (
                        u_next, ub, "up_hub", "up", base - ROW + HUB, None, part,
                    ),
                )

        @pl.when(both(c == HUB, r > 0))
        def _():
            for part in range(2):
                send(
                    lambda: both(c == HUB, r > 0, r < rows - 1),
                    lambda part=part: (
                        u_next, ub, "up_far", "up", base - ROW + LAST, None, part,
                    ),
                )

        @pl.when(c == LAST)
        def _():
            g_in[...] = ub[...]

        @pl.when(c < LAST)
        def _():
            g_in[...] = g_in[...] + dot3(ub[...], sh[...], sl[...])

    upper = dot3(h[1] + g_in[...], dth[1], dtl[1])
    out[1] = upper
    out[0] = dot3(h[0] + vert[1:2, :] * upper, dth[0], dtl[0])

    for cond, args in waits:
        @pl.when(cond())
        def _():
            copy(*args()).wait_send()

    @pl.when(both(c < LAST, has_a))
    def _():
        for b in range(BLOCKS):
            block_a(b).wait_send()

    @pl.when(both(c > 0, has_s))
    def _():
        for b in range(BLOCKS):
            block_s(b).wait_send()


def shards(depth, areas, rhs_field, start_field, inverses, facies, neighbours, lateral_table, vertical_table):
    layers, count, width = rhs_field.shape
    size = width // BLOCKS
    tiles = width // LANES
    field = (layers, count, width)
    matrix = (width, width)
    state = pltpu.VMEM((count, width), F32)

    def blocks():
        return pltpu.VMEM((BLOCKS, size, width), F32)

    def halves():
        return [pltpu.VMEM(matrix, BF16)] * 2

    halo = pltpu.VMEM((count, LANES), F32)
    scratch = (
        [pltpu.SMEM(lateral_table.shape[::-1], F32), pltpu.SMEM(vertical_table.shape, F32)]
        + [pltpu.VMEM(facies.shape, jnp.int32), pltpu.VMEM(neighbours.shape[::-1], jnp.int32)]
        + [pltpu.VMEM(field, F32)] * 2
        + [pltpu.VMEM((layers,) + matrix, F32)]
        + [pltpu.VMEM((layers,) + matrix, BF16)] * 4
        + halves() * 2
        + [blocks()] + halves() + [blocks()]
        + [blocks()] + halves() + [blocks()]
        + halves() * 2
        + [pltpu.VMEM((layers, tiles, 3 * LANES, LANES), BF16)] * 2
        + [pltpu.VMEM((neighbours.shape[1], layers, width), F32)]
        + [pltpu.VMEM((layers, width), F32)] * 2
        + [halo] * 4
        + [pltpu.VMEM((2, count, LANES), F32)] * 2
        + [state] * 2
        + [pltpu.VMEM(field, F32)] + [state] * 6
        + [state] * 3
        + [pltpu.VMEM(field, F32)] * 2
        + [state] * 3
        + [pltpu.VMEM((6, count, width), F32)] + [state]
        + [state] * 4
        + [
            pltpu.SemaphoreType.DMA((7 + tiles,)),
            pltpu.SemaphoreType.DMA((len(SENDS), 2)),
            pltpu.SemaphoreType.DMA((len(RECVS), 2)),
        ]
        + [pltpu.SemaphoreType.DMA((BLOCKS,))] * 4
    )
    vmem = pl.BlockSpec(memory_space=pltpu.VMEM)
    hbm = pl.BlockSpec(memory_space=pl.ANY)
    return pl.pallas_call(
        functools.partial(kernel, depth, areas),
        out_shape=pltpu.VMEM(field, F32),
        in_specs=[hbm] * 7,
        out_specs=vmem,
        scratch_shapes=scratch,
        compiler_params=pltpu.CompilerParams(
            collective_id=0, has_side_effects=True, vmem_limit_bytes=60 * 1024 * 1024
        ),
        name="sweep",
    )(lateral_table.T, vertical_table, facies, neighbours.T, rhs_field, start_field, inverses)


def solution(mesh):
    return jax.shard_map(
        functools.partial(shards, mesh.shape["depth"], mesh.shape["area"]),
        mesh=mesh,
        in_specs=(
            P("depth", None, "area"),
            P("depth", None, "area"),
            P("depth", "area", None),
            P("depth", "area"),
            P("area", None),
            P(),
            P(),
        ),
        out_specs=P("depth", None, "area"),
        check_vma=False,
    )
```

```python
import functools

import jax
import jax.numpy as jnp
from jax import lax
from jax.experimental import pallas as pl
from jax.experimental.pallas import tpu as pltpu
from jax.sharding import PartitionSpec as P

MESH = pl.DeviceIdType.MESH
F32 = jnp.float32
BF16 = jnp.bfloat16
HW = 64
LANES = 128
ROW = 8
LAST = ROW - 1
HUB = 3
SPOKES = (7, 1, 5)
OUTER = (6, 0, 4)
BLOCKS = 8

SENDS = (
    "start_right", "start_left", "below", "f_next", "q_next", "q_far", "q_relay", "down_hub",
    "down_far", "down1", "down5", "down2", "down_pair", "y_right",
    "y_left", "w_pair", "w_hub", "g_prev", "up_hub", "up_far",
    "up1", "up5", "up2", "up_pair",
)
RECVS = (
    "start_lo", "start_hi", "below", "f", "q", "o", "down",
    "y_lo", "y_hi", "w_pair", "w0", "w1", "w2",
    "w3", "w4", "w5", "g", "up",
)


def split(x):
    high = x.astype(BF16)
    return high, (x - high.astype(F32)).astype(BF16)


def dot3(x, w_high, w_low, transposed=False):
    return dot_halves(*split(x), w_high, w_low, transposed)


def dot_halves(high, low, w_high, w_low, transposed):
    dims = (((1,), (1 if transposed else 0,)), ((), ()))
    rows = high.shape[0]
    both = lax.dot_general(
        jnp.concatenate([high, low], axis=0), w_high, dims, preferred_element_type=F32
    )
    rest = lax.dot_general(high, w_low, dims, preferred_element_type=F32)
    return both[:rows] + both[rows:] + rest


def kernel(
    depth, areas,
    lat_tab_hbm, vert_tab_hbm, facies_hbm, nbrs_hbm, rhs_hbm, start_hbm, inv_hbm,
    out,
    lat_tab, vert_tab, facies, nbrs, rhs, start, inv, dh, dl, dth, dtl, th, tl, tth, ttl, ina, ah, al, aht, alt, outa, ins, sh, sl, outs, bh, bl, mh, ml,
    lat_h, lat_l, wts, wsum, vert, slo, shi, ylo, yhi, to_right, to_left, below_out, below_in,
    g, f_in, f_out, o_buf, o_down, q_in, q_out, eb, e_next, e_in, y, h, p_buf, w_out, w_pair, w_hub, o_up,
    g_in, g_out, ub, u_next,
    local, snd, rcv, snd_a, rcv_a, snd_s, rcv_s,
):
    rows = depth // ROW
    d = lax.axis_index("depth")
    z = lax.axis_index("area")
    r, c = d // ROW, d % ROW
    width = out.shape[2]
    count = out.shape[1]
    tiles = width // LANES
    size = width // BLOCKS
    base = r * ROW
    has_a = r > 0
    has_s = r < rows - 1
    waits = []

    def both(*conds):
        return functools.reduce(jnp.logical_and, conds)

    def half(part):
        return pl.ds(part * (count // 2), count // 2)

    def copy(src, dst, send, recv, depth_id, area_id=None, part=None):
        if part is not None:
            src, dst = src.at[half(part)], dst.at[half(part)]
        return pltpu.make_async_remote_copy(
            src_ref=src,
            dst_ref=dst,
            send_sem=snd.at[SENDS.index(send), part or 0],
            recv_sem=rcv.at[RECVS.index(recv), part or 0],
            device_id=(depth_id, z if area_id is None else area_id),
            device_id_type=MESH,
        )

    def send(cond, args):
        waits.append((cond, args))
        copy(*args()).start()

    def received(dst, recv, part=None):
        copy(dst, dst, SENDS[0], recv, d, None, part).wait_recv()

    def block_a(b):
        return pltpu.make_async_remote_copy(
            src_ref=outa.at[b], dst_ref=ina.at[b], send_sem=snd_a.at[b], recv_sem=rcv_a.at[b],
            device_id=(d + 1, z), device_id_type=MESH,
        )

    def block_s(b):
        return pltpu.make_async_remote_copy(
            src_ref=outs.at[b], dst_ref=ins.at[b], send_sem=snd_s.at[b], recv_sem=rcv_s.at[b],
            device_id=(d - 1, z), device_id_type=MESH,
        )

    loads = [
        pltpu.make_async_copy(start_hbm, start, local.at[0]),
        pltpu.make_async_copy(inv_hbm.at[1], inv.at[1], local.at[1]),
        pltpu.make_async_copy(rhs_hbm, rhs, local.at[2]),
    ]

    def load_rows(i):
        some = pl.ds(pl.multiple_of(i * LANES, LANES), LANES)
        return pltpu.make_async_copy(inv_hbm.at[0, some], inv.at[0, some], local.at[3 + i])

    small = [
        pltpu.make_async_copy(source, target, local.at[3 + tiles + i])
        for i, (source, target) in enumerate(
            ((facies_hbm, facies), (nbrs_hbm, nbrs), (lat_tab_hbm, lat_tab), (vert_tab_hbm, vert_tab))
        )
    ]
    for load in small:
        load.start()
    loads[0].start()
    loads[1].start()
    for i in range(tiles):
        load_rows(i).start()
    loads[2].start()

    barrier = pltpu.get_barrier_semaphore()
    is_spoke = both(c % 2 == 1, c != HUB)
    partners = [
        (d > 0, d - 1, z),
        (d < depth - 1, d + 1, z),
        (z > 0, d, z - 1),
        (z < areas - 1, d, z + 1),
        (is_spoke, base + HUB, z),
        (both(c == HUB, r > 0), d - ROW, z),
        (both(c == HUB, r < rows - 1), d + ROW, z),
        (both(c == HUB, r > 0), d - ROW + (LAST - HUB), z),
        (both(c == HUB, r < rows - 1), d + ROW + (LAST - HUB), z),
        (both(c == LAST, r > 0), d - ROW - (LAST - HUB), z),
        (both(c == LAST, r < rows - 1), d + ROW - (LAST - HUB), z),
        (both(c == LAST, r == 0, r < rows - 1), d + ROW, z),
        (both(c == LAST, r == 1), d - ROW, z),
        (c == LAST, base + 1, z),
        (c == 1, base + LAST, z),
        (both(c % 2 == 0, c != HUB - 1), base + HUB, z),
    ] + [(c == HUB, base + other, z) for other in SPOKES + OUTER]
    for cond, to_depth, to_area in partners:

        @pl.when(cond)
        def _():
            pl.semaphore_signal(
                barrier, inc=1, device_id=(to_depth, to_area), device_id_type=MESH
            )

    for load in small:
        load.wait()
    kinds = facies[...]
    facies_count = lat_tab.shape[1]
    v_rows = jnp.zeros(kinds.shape, F32)
    w_rows = [jnp.zeros(kinds.shape, F32) for _ in range(lat_tab.shape[0])]
    for kind in range(facies_count):
        mask = kinds == kind
        v_rows = jnp.where(mask, vert_tab[kind], v_rows)
        w_rows = [jnp.where(mask, lat_tab[j, kind], w) for j, w in enumerate(w_rows)]
    vert[...] = v_rows
    for j, w in enumerate(w_rows):
        wts[j] = w
    wsum[...] = functools.reduce(jnp.add, w_rows)

    for t in range(tiles):
        lanes = slice(t * LANES, (t + 1) * LANES)
        for k in range(2):
            for first in (0, 2 * LANES + HW):
                lat_h[k, t, first : first + HW, :] = jnp.zeros((HW, LANES), BF16)
                lat_l[k, t, first : first + HW, :] = jnp.zeros((HW, LANES), BF16)
        for first in range(HW, 2 * LANES + HW, HW):
            place = lax.broadcasted_iota(jnp.int32, (HW, LANES), 0) + (first + t * LANES - HW)
            sums = [jnp.zeros((HW, LANES), F32) for _ in range(2)]
            for j in range(nbrs.shape[0]):
                hit = place == nbrs[j : j + 1, lanes]
                for k in range(2):
                    sums[k] = sums[k] + jnp.where(hit, wts[j, k : k + 1, lanes], 0.0)
            for k in range(2):
                high, low = split(sums[k])
                lat_h[k, t, first : first + HW, :] = high
                lat_l[k, t, first : first + HW, :] = low

    def lateral_own(k, v):
        parts = [v[:, t * LANES : (t + 1) * LANES] for t in range(tiles)]
        sums = []
        for t in range(tiles):
            first, end = max(t - 1, 0), min(t + 2, tiles)
            rows_of = slice((first - t + 1) * LANES, (end - t + 1) * LANES)
            x = jnp.concatenate(parts[first:end], axis=1)
            sums.append(dot3(x, lat_h[k, t, rows_of], lat_l[k, t, rows_of]))
        return wsum[k : k + 1, :] * v - jnp.concatenate(sums, axis=1)

    def add_neighbours(field, low, high):
        for k in range(2):
            left, right = low[...], high[...]
            if k == 1:
                left, right = pltpu.roll(left, HW, 1), pltpu.roll(right, HW, 1)
            for t, x, first in ((0, left, 0), (tiles - 1, right, 2 * LANES)):
                lanes = slice(t * LANES, (t + 1) * LANES)
                rows_of = slice(first, first + LANES)
                field[k, :, lanes] = field[k, :, lanes] + dot3(
                    x, lat_h[k, t, rows_of], lat_l[k, t, rows_of]
                )

    loads[0].wait()
    below_out[...] = vert[0:1, :] * start[0]
    partner_count = sum(cond.astype(jnp.int32) for cond, _, _ in partners)
    pl.semaphore_wait(barrier, partner_count)

    has_left, has_right = z > 0, z < areas - 1

    def halo(field, low, high, name, place):
        upper_half = lax.broadcasted_iota(jnp.int32, (count, LANES), 1) >= HW

        @pl.when(has_right)
        def _():
            edge = slice(width - LANES, width)
            to_right[place] = jnp.where(
                upper_half, field[0, :, edge], pltpu.roll(field[1, :, edge], HW, 1)
            )
            send(lambda: has_right, lambda: (
                to_right.at[place], low, name + "_right", name + "_lo", d, z + 1,
            ))

        @pl.when(has_left)
        def _():
            to_left[place] = jnp.where(
                upper_half, pltpu.roll(field[1, :, :LANES], HW, 1), field[0, :, :LANES]
            )
            send(lambda: has_left, lambda: (
                to_left.at[place], high, name + "_left", name + "_hi", d, z - 1,
            ))

        @pl.when(jnp.logical_not(has_left))
        def _():
            low[...] = jnp.zeros(low.shape, F32)

        @pl.when(jnp.logical_not(has_right))
        def _():
            high[...] = jnp.zeros(high.shape, F32)

    def halo_received(low, high, name):
        @pl.when(has_left)
        def _():
            received(low, name + "_lo")

        @pl.when(has_right)
        def _():
            received(high, name + "_hi")

    halo(start, slo, shi, "start", 0)

    @pl.when(d > 0)
    def _():
        send(lambda: d > 0, lambda: (below_out, below_in, "below", "below", d - 1))

    def split_layer(k):
        def body(i, _):
            some = pl.ds(pl.multiple_of(i * LANES, LANES), LANES)
            high, low = split(inv[k, some, :])
            dh[k, some, :] = high
            dl[k, some, :] = low
            return 0

        lax.fori_loop(0, tiles, body, 0)

    per_tile = LANES // size

    def scaled_rows(some):
        scale = jnp.transpose(jnp.broadcast_to(vert[0:1, some], (LANES, LANES)))
        return inv[0, some, :] * vert[1:2, :] * jnp.concatenate([scale] * tiles, axis=1)

    def compose(i, _):
        load_rows(i).wait()
        some = pl.ds(pl.multiple_of(i * LANES, LANES), LANES)
        product = dot3(scaled_rows(some), dh[1], dl[1])
        high, low = split(product)
        th[some, :] = high
        tl[some, :] = low
        for part in range(per_tile):
            outa[i * per_tile + part] = product[part * size : (part + 1) * size]

        @pl.when(both(c == 0, has_a))
        def _():
            for part in range(per_tile):
                block_a(i * per_tile + part).start()

        return 0

    def turn(i, _):
        some = pl.ds(pl.multiple_of(i * LANES, LANES), LANES)
        tth[:, some] = jnp.transpose(th[some, :])
        ttl[:, some] = jnp.transpose(tl[some, :])
        return 0

    def halves_of_left(i, _):
        load_rows(i).wait()
        some = pl.ds(pl.multiple_of(i * LANES, LANES), LANES)
        high, low = split(scaled_rows(some))
        sh[some, :] = high
        sl[some, :] = low
        return 0

    def compose_turned(i, _):
        some = pl.ds(pl.multiple_of(i * LANES, LANES), LANES)
        product = dot3(jnp.transpose(inv[1, :, some]), sh[...], sl[...], True)
        for part in range(per_tile):
            outs[i * per_tile + part] = product[part * size : (part + 1) * size]
            block_s(i * per_tile + part).start()
        high, low = split(product)
        tth[some, :] = high
        ttl[some, :] = low
        th[:, some] = jnp.transpose(high)
        tl[:, some] = jnp.transpose(low)
        return 0

    starts_s = both(c == LAST, has_s)
    loads[1].wait()

    @pl.when(starts_s)
    def _():
        lax.fori_loop(0, tiles, halves_of_left, 0)
        lax.fori_loop(0, tiles, compose_turned, 0)
        split_layer(1)

    @pl.when(jnp.logical_not(starts_s))
    def _():
        split_layer(1)
        lax.fori_loop(0, tiles, compose, 0)

    def own_part():
        split_layer(0)
        loads[2].wait()
        g[0] = rhs[0] - lateral_own(0, start[0]) + vert[1:2, :] * start[1]
        g[1] = rhs[1] - lateral_own(1, start[1])
        halo_received(slo, shi, "start")
        add_neighbours(g, slo, shi)

        @pl.when(d < depth - 1)
        def _():
            received(below_in, "below")
            g[1] = g[1] + below_in[...]

        first = dot3(g[0], dh[0], dl[0])
        o_buf[...] = dot3(g[1] + vert[1:2, :] * first, dh[1], dl[1])

        @pl.when(c == 0)
        def _():
            f_in[...] = jnp.zeros(f_in.shape, F32)
            f_out[...] = o_buf[...]

    step_a = (c // 2) * 4 + c % 2
    last = LAST - c
    step_s = (last // 2) * 4 + last % 2

    def next_f(part):
        return f_out, f_in, "f_next", "f", d + 1, None, part

    def next_q():
        return q_out, q_in, "q_next", "q", d + 1

    def far_q():
        return q_out, q_in, "q_far", "q", base + 1

    def relay_q():
        return q_in, o_down, "q_relay", "o", base + HUB

    def first_offset(part):
        return f_out, eb, "down_hub", "down", base + ROW + HUB, None, part

    def first_far(part):
        return f_out, eb, "down_far", "down", base + ROW + LAST, None, part

    step_f = jnp.where(has_a, jnp.maximum(step_a + 1, 2), jnp.maximum(step_a, 1))
    has_q = both(has_a, has_s)
    step_q = jnp.where(c == HUB + 1, 3, jnp.where(c == HUB + 2, 4, jnp.where(c == 1, 11, c + 3)))
    step_own = jnp.where(has_a, jnp.where(c <= 1, 2, 3), 1)

    def slot(s, _):
        @pl.when(both(c > 0, has_a, s >= step_a, s < step_a + BLOCKS))
        def _():
            b = s - step_a
            some = pl.ds(pl.multiple_of(b * size, size), size)
            block_a(b).wait_recv()
            high, low = split(ina[b])
            ah[some, :] = high
            al[some, :] = low

            @pl.when(c < LAST)
            def _():
                product = dot_halves(high, low, th[...], tl[...], False)
                outa[b] = product
                block_a(b).start()

                @pl.when(c == HUB)
                def _():
                    high, low = split(product)
                    bh[some, :] = high
                    bl[some, :] = low

        @pl.when(s == step_own)
        def _():
            own_part()

        @pl.when(s == step_f)
        def _():
            for part in range(2):
                some = half(part)

                @pl.when(c > 0)
                def _():
                    received(f_in, "f", part)
                    f_out[some] = dot3(f_in[some], th[...], tl[...]) + o_buf[some]

                @pl.when(c < LAST)
                def _():
                    copy(*next_f(part)).start()

                @pl.when(both(c == LAST, r == 0, r < rows - 1))
                def _():
                    copy(*first_offset(part)).start()

            @pl.when(both(c == LAST, r == 0, r < rows - 1))
            def _():
                for part in range(2):
                    copy(*first_far(part)).start()

        @pl.when(both(has_q, s == step_q))
        def _():
            @pl.when(c == HUB + 1)
            def _():
                q_out[...] = o_buf[...]

            @pl.when(c > HUB + 1)
            def _():
                received(q_in, "q")
                q_out[...] = dot3(q_in[...], th[...], tl[...]) + o_buf[...]

            @pl.when(both(c > HUB, c < LAST))
            def _():
                copy(*next_q()).start()

            @pl.when(c == LAST)
            def _():
                copy(*far_q()).start()

            @pl.when(c == 1)
            def _():
                received(q_in, "q")
                copy(*relay_q()).start()

        @pl.when(both(s == 4, jnp.logical_not(starts_s)))
        def _():
            lax.fori_loop(0, tiles, turn, 0)

        @pl.when(both(c < LAST, has_s, s >= step_s, s < step_s + BLOCKS))
        def _():
            b = s - step_s
            some = pl.ds(pl.multiple_of(b * size, size), size)
            block_s(b).wait_recv()
            high, low = split(ins[b])
            sh[some, :] = high
            sl[some, :] = low

            @pl.when(c == LAST - 1)
            def _():
                outs[b] = dot_halves(high, low, th[...], tl[...], True)
                block_s(b).start()

            @pl.when(both(c > 0, c < LAST - 1))
            def _():
                outs[b] = dot_halves(high, low, tth[...], ttl[...], False)
                block_s(b).start()

        @pl.when(both(s > 5, s < 8))
        def _():
            k = s - 6
            for t in range(tiles):
                lanes = slice(t * LANES, (t + 1) * LANES)
                dth[k, :, lanes] = jnp.transpose(dh[k, lanes, :])
                dtl[k, :, lanes] = jnp.transpose(dl[k, lanes, :])

        return 0

    lax.fori_loop(0, (ROW // 2 - 1) * 4 + 1 + BLOCKS, slot, 0)
    waits.append((lambda: both(has_q, c > HUB, c < LAST), next_q))
    waits.append((lambda: both(has_q, c == LAST), far_q))
    waits.append((lambda: both(has_q, c == 1), relay_q))
    for part in range(2):
        waits.append((lambda: c < LAST, functools.partial(next_f, part)))
        for late in (first_offset, first_far):
            waits.append(
                (lambda: both(c == LAST, r == 0, r < rows - 1), functools.partial(late, part))
            )

    def spread(cond, buf, name, part):
        @pl.when(c == HUB)
        def _():
            for spoke in (1, 5, HUB - 1):
                send(
                    lambda: both(cond(), c == HUB),
                    lambda spoke=spoke: (
                        buf, buf, name + str(spoke), name, base + spoke, None, part,
                    ),
                )

        @pl.when(is_spoke)
        def _():
            send(
                lambda: both(cond(), is_spoke),
                lambda: (buf, buf, name + "_pair", name, d - 1, None, part),
            )

    @pl.when(r == 0)
    def _():
        e_in[...] = f_in[...]

    @pl.when(r > 0)
    def _():
        @pl.when(both(c == HUB, r < rows - 1))
        def _():
            received(o_down, "o")

        for part in range(2):
            some = half(part)
            received(eb, "down", part)
            spread(lambda: r > 0, eb, "down", part)

            @pl.when(both(c == HUB, r < rows - 1))
            def _():
                across = dot3(eb[some], bh[...], bl[...]) + f_out[some]
                e_next[some] = dot3(across, sh[...], sl[...], True) + o_down[some]
                send(
                    lambda: both(c == HUB, r > 0, r < rows - 1),
                    lambda part=part: (
                        e_next, eb, "down_hub", "down", base + ROW + HUB, None, part,
                    ),
                )

        @pl.when(both(c == HUB, r < rows - 1))
        def _():
            for part in range(2):
                send(
                    lambda: both(c == HUB, r > 0, r < rows - 1),
                    lambda part=part: (
                        e_next, eb, "down_far", "down", base + ROW + LAST, None, part,
                    ),
                )

            def product(i, _):
                some = pl.ds(pl.multiple_of(i * LANES, LANES), LANES)
                high, low = split(dot_halves(sh[some, :], sl[some, :], bh[...], bl[...], True))
                mh[some, :] = high
                ml[some, :] = low
                return 0

            lax.fori_loop(0, tiles, product, 0)

        @pl.when(c == 0)
        def _():
            e_in[...] = eb[...]

        @pl.when(c > 0)
        def _():
            e_in[...] = dot3(eb[...], ah[...], al[...]) + f_in[...]

    entering = vert[0:1, :] * e_in[...]
    y[0] = dot3(g[0] + entering, dh[0], dl[0])
    y[1] = dot3(g[1] + vert[1:2, :] * y[0], dh[1], dl[1])
    halo(y, ylo, yhi, "y", 1)
    h[0] = rhs[0] - lateral_own(0, y[0]) + entering
    h[1] = rhs[1] - lateral_own(1, y[1]) + vert[1:2, :] * y[0]

    @pl.when(both(c > 0, r > 0))
    def _():
        for t in range(tiles):
            lanes = slice(t * LANES, (t + 1) * LANES)
            aht[:, lanes] = jnp.transpose(ah[lanes, :])
            alt[:, lanes] = jnp.transpose(al[lanes, :])

    halo_received(ylo, yhi, "y")
    add_neighbours(h, ylo, yhi)

    def next_g(part):
        return g_out, g_in, "g_prev", "g", d - 1, None, part

    above = dot3(h[1], dth[1], dtl[1])
    p_buf[...] = vert[0:1, :] * dot3(h[0] + vert[1:2, :] * above, dth[0], dtl[0])

    @pl.when(c == LAST)
    def _():
        g_in[...] = jnp.zeros(g_in.shape, F32)
        g_out[...] = p_buf[...]
        for part in range(2):
            copy(*next_g(part)).start()

    @pl.when(r > 0)
    def _():
        @pl.when(c == 0)
        def _():
            w_out[...] = p_buf[...]

        @pl.when(c > 0)
        def _():
            w_out[...] = dot3(p_buf[...], aht[...], alt[...])

        @pl.when(c == HUB - 1)
        def _():
            send(
                lambda: both(r > 0, c == HUB - 1),
                lambda: (w_out, w_pair, "w_pair", "w_pair", d + 1),
            )

        for i, other in enumerate(SPOKES + OUTER):

            @pl.when(c == other)
            def _():
                send(
                    lambda other=other: both(r > 0, c == other),
                    lambda i=i: (w_out, w_hub.at[i], "w_hub", "w" + str(i), base + HUB),
                )

        @pl.when(c == HUB)
        def _():
            received(w_pair, "w_pair")
            own = w_out[...] + w_pair[...]
            for other in range(len(SPOKES + OUTER)):
                received(w_hub.at[other], "w" + str(other))
                own = own + w_hub[other]
            o_up[...] = own

            @pl.when(r == rows - 1)
            def _():
                for name, to in (("up_hub", HUB), ("up_far", LAST)):
                    for part in range(2):
                        send(
                            lambda: both(c == HUB, r > 0, r == rows - 1),
                            lambda name=name, to=to, part=part: (
                                o_up, ub, name, "up", base - ROW + to, None, part,
                            ),
                        )

    @pl.when(c < LAST)
    def _():
        for part in range(2):
            some = half(part)
            received(g_in, "g", part)

            @pl.when(c > 0)
            def _():
                g_out[some] = dot3(g_in[some], tth[...], ttl[...]) + p_buf[some]
                copy(*next_g(part)).start()

    for part in range(2):
        waits.append((lambda: c > 0, functools.partial(next_g, part)))

    @pl.when(r < rows - 1)
    def _():
        for part in range(2):
            some = half(part)
            received(ub, "up", part)
            spread(lambda: r < rows - 1, ub, "up", part)

            @pl.when(both(c == HUB, r > 0))
            def _():
                u_next[some] = dot3(ub[some], mh[...], ml[...]) + o_up[some]
                send(
                    lambda: both(c == HUB, r > 0, r < rows - 1),
                    lambda part=part: (
                        u_next, ub, "up_hub", "up", base - ROW + HUB, None, part,
                    ),
                )

        @pl.when(both(c == HUB, r > 0))
        def _():
            for part in range(2):
                send(
                    lambda: both(c == HUB, r > 0, r < rows - 1),
                    lambda part=part: (
                        u_next, ub, "up_far", "up", base - ROW + LAST, None, part,
                    ),
                )

        @pl.when(c == LAST)
        def _():
            g_in[...] = ub[...]

        @pl.when(c < LAST)
        def _():
            g_in[...] = g_in[...] + dot3(ub[...], sh[...], sl[...])

    upper = dot3(h[1] + g_in[...], dth[1], dtl[1])
    out[1] = upper
    out[0] = dot3(h[0] + vert[1:2, :] * upper, dth[0], dtl[0])

    for cond, args in waits:
        @pl.when(cond())
        def _():
            copy(*args()).wait_send()

    @pl.when(both(c < LAST, has_a))
    def _():
        for b in range(BLOCKS):
            block_a(b).wait_send()

    @pl.when(both(c > 0, has_s))
    def _():
        for b in range(BLOCKS):
            block_s(b).wait_send()


def shards(depth, areas, rhs_field, start_field, inverses, facies, neighbours, lateral_table, vertical_table):
    layers, count, width = rhs_field.shape
    size = width // BLOCKS
    tiles = width // LANES
    field = (layers, count, width)
    matrix = (width, width)
    state = pltpu.VMEM((count, width), F32)

    def blocks():
        return pltpu.VMEM((BLOCKS, size, width), F32)

    def halves():
        return [pltpu.VMEM(matrix, BF16)] * 2

    halo = pltpu.VMEM((count, LANES), F32)
    scratch = (
        [pltpu.SMEM(lateral_table.shape[::-1], F32), pltpu.SMEM(vertical_table.shape, F32)]
        + [pltpu.VMEM(facies.shape, jnp.int32), pltpu.VMEM(neighbours.shape[::-1], jnp.int32)]
        + [pltpu.VMEM(field, F32)] * 2
        + [pltpu.VMEM((layers,) + matrix, F32)]
        + [pltpu.VMEM((layers,) + matrix, BF16)] * 4
        + halves() * 2
        + [blocks()] + halves() * 2 + [blocks()]
        + [blocks()] + halves() + [blocks()]
        + halves() * 2
        + [pltpu.VMEM((layers, tiles, 3 * LANES, LANES), BF16)] * 2
        + [pltpu.VMEM((neighbours.shape[1], layers, width), F32)]
        + [pltpu.VMEM((layers, width), F32)] * 2
        + [halo] * 4
        + [pltpu.VMEM((2, count, LANES), F32)] * 2
        + [state] * 2
        + [pltpu.VMEM(field, F32)] + [state] * 6
        + [state] * 3
        + [pltpu.VMEM(field, F32)] * 2
        + [state] * 3
        + [pltpu.VMEM((6, count, width), F32)] + [state]
        + [state] * 4
        + [
            pltpu.SemaphoreType.DMA((7 + tiles,)),
            pltpu.SemaphoreType.DMA((len(SENDS), 2)),
            pltpu.SemaphoreType.DMA((len(RECVS), 2)),
        ]
        + [pltpu.SemaphoreType.DMA((BLOCKS,))] * 4
    )
    vmem = pl.BlockSpec(memory_space=pltpu.VMEM)
    hbm = pl.BlockSpec(memory_space=pl.ANY)
    return pl.pallas_call(
        functools.partial(kernel, depth, areas),
        out_shape=pltpu.VMEM(field, F32),
        in_specs=[hbm] * 7,
        out_specs=vmem,
        scratch_shapes=scratch,
        compiler_params=pltpu.CompilerParams(
            collective_id=0, has_side_effects=True, vmem_limit_bytes=60 * 1024 * 1024
        ),
        name="sweep",
    )(lateral_table.T, vertical_table, facies, neighbours.T, rhs_field, start_field, inverses)


def solution(mesh):
    return jax.shard_map(
        functools.partial(shards, mesh.shape["depth"], mesh.shape["area"]),
        mesh=mesh,
        in_specs=(
            P("depth", None, "area"),
            P("depth", None, "area"),
            P("depth", "area", None),
            P("depth", "area"),
            P("area", None),
            P(),
            P(),
        ),
        out_specs=P("depth", None, "area"),
        check_vma=False,
    )
```
